32 devices in a mesh: ocn: 4 (over z), grp: 8 (over y, x, core).
Axes of the slice: x: 2, y: 2, z: 4, core: 2. Of those that a mesh axis runs over, the one named last changes fastest.
Arguments:
- tracers: float32 [2, 32, 256, 1024], P(None, None, 'grp', 'ocn'), may hold values from -6 to 6
- velocity: float32 [2, 32, 256, 1024], P(None, None, 'grp', 'ocn'), may hold values from -3 to 3
- remap_weights: bfloat16 [256, 8, 128, 128], P('grp'), may hold values from -0.25 to 0.25
- remap_blocks: int32 [256, 8], P('grp'), may hold values from 0 to 2047
- remap_count: int32 [256], P('grp'), may hold values from 1 to 8, as said below
- ice_velocity: float32 [2, 32768], P(None, 'grp'), may hold values from -3 to 3
- ice_mass_rate: float32 [32768], P('grp'), may hold values from 0.5 to 4
- ice_strength: float32 [32768], P('grp'), may hold values from 0.5 to 8
- wind_stress: float32 [2, 32768], P(None, 'grp'), may hold values from -6 to 6
Outputs:
- tracers_next: float32 [2, 32, 256, 1024], P(None, None, 'grp', 'ocn')
- surface_flux: float32 [3, 256, 1024], P(None, 'grp', 'ocn')
- ice_final: float32 [2, 32768], P(None, 'grp')
The draws below stay inside these ranges and needn't reach their ends.
Inputs may be any that keep to these rules, and one draw needn't show every extreme that they name: `remap_count`: every ice block has at least one live entry. The ice blocks of the first and of the last index of grp have 7 or 8 live entries; all others have 1 or 2.
All inputs are finite; a program needn't handle non-finite values.
Results may differ from the reference program's by a relative error of at most 0.0006.
The reference program's roundings to bfloat16 on the way (of `surface` and `ice_flux`) count: a program that leaves them out, or rounds other values in their place, can miss the bound.
Values may be sent and summed in bfloat16 or wider, within the bound.
No kernel may reach another device: no remote copies, remote signals or barrier semaphores. Data moves between devices by JAX's collectives and lax.ppermute only.
A program may use at most 128 MiB of HBM per device.

```python
import math
import jax
import jax.numpy as jnp
from jax import lax

L = 32
CY = 32
CX = 256
BS = 128
K = 8
IBD = 32
ITERS = 4
DEPTH = 3
NY = 256
NX = 1024
BPD = 64
OB = 2048
ICE_BLOCKS = 256
ICE_CELLS = 32768
N_OCN = 4
N_GRP = 8


def draw_remap_count(key, part):
    busy_key = jax.random.fold_in(key, 11)
    drawn_key = jax.random.fold_in(key, 23)
    busy = jax.random.randint(busy_key, (ICE_BLOCKS,), K - 1, K + 1)
    drawn = jax.random.randint(drawn_key, (ICE_BLOCKS,), 1, max(2, K // 4) + 1)
    position = jnp.arange(ICE_BLOCKS)
    polar = (position < IBD) | (position >= ICE_BLOCKS - IBD)
    return jnp.where(polar, busy, drawn).astype(jnp.int32)


def draw_wind_stress(key, part):
    noise_key = jax.random.fold_in(key, 37)
    place = jnp.arange(ICE_CELLS, dtype=jnp.float32) / max(ICE_CELLS - 1, 1)
    ramp = 1.0 + 3.0 * place
    noise = jax.random.normal(noise_key, (2, ICE_CELLS), jnp.float32) * 0.5
    return jnp.clip(noise * ramp[None, :], -6.0, 6.0).astype(jnp.float32)


def plant(result, rng, low, largest):
    shape = result.shape
    spot = [jax.random.randint(jax.random.fold_in(rng, axis), (), 0, shape[axis]) for axis in range(len(shape))]
    result = result.at[tuple(spot)].set(low)
    longest = shape.index(max(shape))
    spot[longest] = (spot[longest] + 1) % shape[longest]
    return result.at[tuple(spot)].set(largest)


def shard_levels(own_key, shape, cuts, low, largest):
    loudness, own = 1.0, jax.random.fold_in(own_key, 6)
    for dim, parts in cuts:
        heights = jnp.exp(jax.random.uniform(jax.random.fold_in(own, dim), (parts,), jnp.float32, low / len(cuts), largest / len(cuts)))
        loudness = loudness * jnp.repeat(heights, shape[dim] // parts).reshape([-1 if axis == dim else 1 for axis in range(len(shape))])
    return loudness


def scatter_about(stream_key, extent, width, limit, split=(), kind=jnp.bfloat16):
    array = jax.random.normal(stream_key, extent, jnp.float32) * width
    if len(split) > 0:
        array = shard_levels(stream_key, extent, split, -0.22, 0.18) * array
    return jnp.clip(array, min=-limit, max=limit).astype(kind)


def setup_inputs(seed: int = 0) -> dict:
    arg_keys = jax.random.split(jax.random.key(seed), 10)
    tracers = scatter_about(arg_keys[0], (2, L, NY, NX), 1.0, 6.0, ((2, 8), (3, 4)), jnp.float32)
    velocity = scatter_about(arg_keys[1], (2, L, NY, NX), 0.5, 3.0, ((2, 8), (3, 4)), jnp.float32)
    remap_weights = scatter_about(arg_keys[2], (ICE_BLOCKS, K, BS, BS), (BS * K // 2) ** -0.5, 0.25, ((0, 8),))
    remap_blocks = plant(jax.random.randint(arg_keys[3], (ICE_BLOCKS, K), 0, OB), jax.random.fold_in(arg_keys[3], 1), 0, OB - 1).astype(jnp.int32)
    remap_count = draw_remap_count(jax.random.fold_in(arg_keys[9], 71), 0)
    ice_velocity = scatter_about(arg_keys[5], (2, ICE_CELLS), 0.5, 3.0, ((1, 8),), jnp.float32)
    ice_mass_rate = jnp.clip(jnp.exp(math.log(4.0) - 2.0794415 * jax.random.uniform(arg_keys[6], (ICE_CELLS,), jnp.float32) ** shard_levels(arg_keys[6], (ICE_CELLS,), ((0, 8),), -0.2, 0.2)), 0.5, 4.0)
    ice_strength = jnp.clip(jnp.exp(math.log(8.0) - 2.7725887 * jax.random.uniform(arg_keys[7], (ICE_CELLS,), jnp.float32) ** shard_levels(arg_keys[7], (ICE_CELLS,), ((0, 8),), -0.2, 0.2)), 0.5, 8.0)
    wind_stress = draw_wind_stress(jax.random.fold_in(arg_keys[9], 71), 0)
    return {"tracers": tracers, "velocity": velocity, "remap_weights": remap_weights, "remap_blocks": remap_blocks, "remap_count": remap_count, "ice_velocity": ice_velocity, "ice_mass_rate": ice_mass_rate, "ice_strength": ice_strength, "wind_stress": wind_stress}


def pack_surface(fields):
    count = fields.shape[0]
    grid = fields.reshape(count, N_GRP, CY, N_OCN, CX).transpose(3, 1, 0, 2, 4)
    grid = grid.reshape(N_OCN, N_GRP, count, BPD, BS).transpose(0, 1, 3, 2, 4)
    return grid.reshape(OB, count, BS)

def unpack_surface(blocks):
    count = blocks.shape[1]
    grid = blocks.reshape(N_OCN, N_GRP, BPD, count, BS).transpose(3, 1, 0, 2, 4)
    grid = grid.reshape(count, N_GRP, N_OCN, CY, CX).transpose(0, 1, 3, 2, 4)
    return grid.reshape(count, NY, NX)

def picard_map(u, base, rate, strength):
    padded = jnp.pad(u, ((0, 0), (1, 1)))
    left = padded[:, :-2]
    right = padded[:, 2:]
    strain = 0.5 * (right - left)
    zeta = strength / (2.0 * jnp.sqrt(lax.optimization_barrier(jnp.sum(strain * strain, axis=0)) + 0.25))
    return (base + zeta * (left + right)) / (rate + 1.0 + 2.0 * zeta)

def reference(tracers, velocity, remap_weights, remap_blocks, remap_count, ice_velocity, ice_mass_rate, ice_strength, wind_stress):
    live = (jnp.arange(K)[None, :] < remap_count[:, None]).astype(jnp.float32)
    surface = jnp.stack([tracers[0, 0], tracers[1, 0], velocity[0, 0], velocity[1, 0]]).astype(jnp.bfloat16)
    blocks = pack_surface(surface)
    source = blocks[remap_blocks].astype(jnp.float32) * live[:, :, None, None]
    weights = remap_weights.astype(jnp.float32)
    remapped = jnp.einsum('rkij,rkfj->rfi', weights, source, precision=lax.Precision.HIGHEST)
    remapped = remapped.transpose(1, 0, 2).reshape(4, ICE_CELLS)
    base = ice_mass_rate * ice_velocity + wind_stress + remapped[2:4]
    total = 2.0 * ICE_CELLS
    current = ice_velocity
    gvals = []
    fvals = []
    for step in range(ITERS):
        gnew = picard_map(current, base, ice_mass_rate, ice_strength)
        gvals.append(gnew)
        fvals.append(gnew - current)
        if step == 0:
            current = gnew
            continue
        depth = min(step, DEPTH)
        diffs = jnp.stack([fvals[j] - fvals[j - 1] for j in range(step - depth + 1, step + 1)])
        gdiffs = jnp.stack([gvals[j] - gvals[j - 1] for j in range(step - depth + 1, step + 1)])
        norms = jnp.sqrt(lax.optimization_barrier(jnp.sum(diffs * diffs, axis=(1, 2))) / total + 1e-06)
        gram = jnp.einsum('aij,bij->ab', diffs, diffs, precision=lax.Precision.HIGHEST) / total
        gram = gram / (norms[:, None] * norms[None, :])
        rhs = jnp.einsum('aij,ij->a', diffs, fvals[step], precision=lax.Precision.HIGHEST) / total / norms
        coef = jnp.linalg.solve(gram + 0.1 * jnp.eye(depth, dtype=jnp.float32), rhs)
        current = gnew - jnp.einsum('a,aij->ij', coef / norms, gdiffs, precision=lax.Precision.HIGHEST)
    ice_final = current
    heat = 0.5 * (-0.05 * remapped[1] - remapped[0])
    ice_flux = jnp.concatenate([ice_final - remapped[2:4], heat[None]], axis=0).astype(jnp.bfloat16)
    flux_blocks = ice_flux.astype(jnp.float32).reshape(3, ICE_BLOCKS, BS).transpose(1, 0, 2)
    contrib = jnp.einsum('rkij,rfi->rkfj', weights, flux_blocks, precision=lax.Precision.HIGHEST)
    contrib = (contrib * live[:, :, None, None]).reshape(ICE_BLOCKS * K, 3, BS)
    summed = jax.ops.segment_sum(contrib, remap_blocks.reshape(-1), num_segments=OB)
    surface_flux = unpack_surface(summed)
    padded = jnp.pad(tracers, ((0, 0), (1, 1), (1, 1), (1, 1)))
    centre = padded[:, 1:-1, 1:-1, 1:-1]
    east = padded[:, 1:-1, 1:-1, 2:]
    west = padded[:, 1:-1, 1:-1, :-2]
    north = padded[:, 1:-1, 2:, 1:-1]
    south = padded[:, 1:-1, :-2, 1:-1]
    upper = padded[:, :-2, 1:-1, 1:-1]
    lower = padded[:, 2:, 1:-1, 1:-1]
    advect = velocity[0][None] * (east - west) * 0.5 + velocity[1][None] * (north - south) * 0.5
    tracers_next = centre + 0.2 * (east + west + north + south - 4.0 * centre) - 0.5 * advect + 0.2 * (upper + lower - 2.0 * centre)
    tracers_next = tracers_next.at[0, 0].add(0.5 * surface_flux[2])
    return (tracers_next, surface_flux, ice_final)
```

```python
import jax
import jax.numpy as jnp
from jax import lax
from jax.experimental import pallas as pl
from jax.experimental.pallas import tpu as pltpu
from jax.sharding import PartitionSpec as P

BS = 128
ITERS = 4
DEPTH = 3
UNROLL = 8
FWD_SLOTS = 32
BWD_SLOTS = 64
F32 = jnp.float32
BF16 = jnp.bfloat16


VM = pl.BlockSpec(memory_space=pltpu.VMEM)
SM = pl.BlockSpec(memory_space=pltpu.SMEM)
ANY = pl.BlockSpec(memory_space=pl.ANY)


def params(**kw):
    return pltpu.CompilerParams(vmem_limit_bytes=48 * 1024 * 1024, **kw)


def surface_kernel(t_ref, v_ref, out_ref):
    height, across = t_ref.shape[2], t_ref.shape[3]
    for f in range(4):
        src = t_ref if f < 2 else v_ref
        for h in range(across // BS):
            out_ref[f, h * height : (h + 1) * height, :] = src[
                f % 2, 0, :, h * BS : (h + 1) * BS
            ].astype(BF16)


def pack_surface(tracers, velocity):
    height, across = tracers.shape[2:]
    spec = pl.BlockSpec((2, 1, height, across), lambda i: (0, 0, 0, 0))
    nbl = height * across // BS
    return pl.pallas_call(
        surface_kernel,
        grid=(1,),
        in_specs=[spec, spec],
        out_specs=pl.BlockSpec((4, nbl, BS), lambda i: (0, 0, 0)),
        out_shape=jax.ShapeDtypeStruct((4, nbl, BS), BF16),
        name="surface",
    )(tracers, velocity)


def edges_kernel(t_ref, row0_ref, rown_ref, col0_ref, coln_ref):
    step = pl.program_id(0)
    lc, height, across = t_ref.shape[1:]
    levels = lc * pl.num_programs(0)
    lane = lax.broadcasted_iota(jnp.int32, (height, BS), 1)

    @pl.when(step == 0)
    def _():
        col0_ref[...] = jnp.zeros_like(col0_ref)
        coln_ref[...] = jnp.zeros_like(coln_ref)

    first = col0_ref[...]
    last = coln_ref[...]
    for t in range(2):
        for i in range(lc):
            c = t * levels + step * lc + i
            first = jnp.where(lane == c, pltpu.roll(t_ref[t, i, :, :BS], c, 1), first)
            last = jnp.where(
                lane == c, pltpu.roll(t_ref[t, i, :, across - BS :], (c + 1) % BS, 1), last
            )
            row0_ref[t, i : i + 1, :] = t_ref[t, i, 0:1, :]
            rown_ref[t, i : i + 1, :] = t_ref[t, i, height - 1 : height, :]
    col0_ref[...] = first
    coln_ref[...] = last


def pack_edges(tracers):
    _, levels, height, across = tracers.shape
    lc = 8
    rows = jax.ShapeDtypeStruct((2, levels, across), F32)
    cols = jax.ShapeDtypeStruct((height, BS), F32)
    row_spec = pl.BlockSpec((2, lc, across), lambda i: (0, i, 0))
    col_spec = pl.BlockSpec((height, BS), lambda i: (0, 0))
    return pl.pallas_call(
        edges_kernel,
        grid=(levels // lc,),
        in_specs=[pl.BlockSpec((2, lc, height, across), lambda i: (0, i, 0, 0))],
        out_specs=[row_spec, row_spec, col_spec, col_spec],
        out_shape=[rows, rows, cols, cols],
        name="edges",
    )(tracers)


def stencil_kernel(t_ref, up_ref, dn_ref, v_ref, north_ref, south_ref, east_ref, west_ref, out_ref):
    step = pl.program_id(0)
    steps = pl.num_programs(0)
    lc, height, across = t_ref.shape[1:]
    levels = lc * steps
    lane = lax.broadcasted_iota(jnp.int32, (height, across), 1)
    row = lax.broadcasted_iota(jnp.int32, (height, across), 0)
    pad = jnp.zeros((height, across - BS), F32)
    top = jnp.where(step == 0, 0.0, 1.0)
    bottom = jnp.where(step == steps - 1, 0.0, 1.0)
    for i in range(lc):
        u = v_ref[0, i]
        v = v_ref[1, i]
        for t in range(2):
            c = t * levels + step * lc + i
            x = t_ref[t, i]
            above = up_ref[t, 0] * top if i == 0 else t_ref[t, i - 1]
            below = dn_ref[t, 0] * bottom if i == lc - 1 else t_ref[t, i + 1]
            wcol = jnp.concatenate(
                [pltpu.roll(west_ref[...], (BS - c) % BS, 1), pad], axis=1
            )
            ecol = jnp.concatenate([pad, pltpu.roll(east_ref[...], BS - 1 - c, 1)], axis=1)
            w = jnp.where(lane == 0, wcol, pltpu.roll(x, 1, 1))
            e = jnp.where(lane == across - 1, ecol, pltpu.roll(x, across - 1, 1))
            s = jnp.where(row == 0, south_ref[t, i : i + 1, :], pltpu.roll(x, 1, 0))
            n = jnp.where(row == height - 1, north_ref[t, i : i + 1, :], pltpu.roll(x, height - 1, 0))
            advect = u * (e - w) * 0.5 + v * (n - s) * 0.5
            out_ref[t, i] = (
                x
                + 0.2 * (e + w + n + s - 4.0 * x)
                - 0.5 * advect
                + 0.2 * (above + below - 2.0 * x)
            )


def stencil(tracers, velocity, north, south, east, west):
    _, levels, height, across = tracers.shape
    lc = 8
    main = pl.BlockSpec((2, lc, height, across), lambda i: (0, i, 0, 0))
    up = pl.BlockSpec((2, 1, height, across), lambda i: (0, jnp.maximum(i * lc - 1, 0), 0, 0))
    dn = pl.BlockSpec(
        (2, 1, height, across), lambda i: (0, jnp.minimum(i * lc + lc, levels - 1), 0, 0)
    )
    row_spec = pl.BlockSpec((2, lc, across), lambda i: (0, i, 0))
    col_spec = pl.BlockSpec((height, BS), lambda i: (0, 0))
    return pl.pallas_call(
        stencil_kernel,
        grid=(levels // lc,),
        in_specs=[main, up, dn, main, row_spec, row_spec, col_spec, col_spec],
        out_specs=main,
        out_shape=jax.ShapeDtypeStruct(tracers.shape, F32),
        cost_estimate=pl.CostEstimate(
            flops=120_000_000, bytes_accessed=4 * tracers.size * 4, transcendentals=0
        ),
        name="stencil",
    )(tracers, tracers, tracers, velocity, north, south, east, west)


def stream_weights(list_ref, groups, w_hbm, buf, sems, compute, prime=True):
    slots = buf.shape[0]

    def copy(i, slot):
        return pltpu.make_async_copy(w_hbm.at[list_ref[i]], buf.at[slot], sems.at[slot])

    def start():
        for s in range(slots // UNROLL):

            @pl.when(s < groups)
            def _():
                for q in range(UNROLL):
                    copy(s * UNROLL + q, s * UNROLL + q).start()

    def loop():
        def body(g, carry):
            base = g * UNROLL
            slot = lax.rem(g, slots // UNROLL) * UNROLL
            for q in range(UNROLL):
                copy(base + q, slot + q).wait()
            compute(base, slot)

            @pl.when(g + slots // UNROLL < groups)
            def _():
                for q in range(UNROLL):
                    copy(base + slots + q, slot + q).start()

            return carry

        lax.fori_loop(0, groups, body, 0)

    return start, loop


def forward_kernel(code_ref, surf_ref, w_hbm, out_ref, list_ref, rows, acc, buf, sems):
    entries = code_ref.shape[0]
    ice = acc.shape[0]
    per_block = entries // ice
    nbl = surf_ref.shape[1]

    def scan(i, n):
        for q in range(8):
            e = i * 8 + q
            list_ref[n] = e
            n = n + jnp.where(code_ref[e] >= 0, 1, 0)
        return n

    count = lax.fori_loop(0, entries // 8, scan, 0)
    for q in range(UNROLL):
        list_ref[count + q] = 0
    list_ref[entries + UNROLL] = count
    groups = lax.div(count + UNROLL - 1, UNROLL)
    first = lax.broadcasted_iota(jnp.int32, (4, BS), 0)

    def compute(base, slot):
        for q in range(UNROLL):
            e = list_ref[base + q]
            at = jnp.maximum(code_ref[e], 0)
            r0 = jnp.broadcast_to(rows[pl.ds(at, 1), :], (4, BS))
            r1 = jnp.broadcast_to(rows[pl.ds(at + nbl, 1), :], (4, BS))
            r2 = jnp.broadcast_to(rows[pl.ds(at + 2 * nbl, 1), :], (4, BS))
            r3 = jnp.broadcast_to(rows[pl.ds(at + 3 * nbl, 1), :], (4, BS))
            s = jnp.where(first == 0, r0, jnp.where(first == 1, r1, jnp.where(first == 2, r2, r3)))
            s = jnp.where(base + q < count, s, 0.0).astype(BF16)
            part = lax.dot_general(
                s, buf[slot + q], (((1,), (1,)), ((), ())), preferred_element_type=F32
            )
            r = lax.div(e, per_block)
            acc[r] = acc[r] + part

    start, loop = stream_weights(list_ref, groups, w_hbm, buf, sems, compute)
    start()
    planes = surf_ref.shape[0]
    for p in range(planes):
        rows[p * nbl : (p + 1) * nbl, :] = surf_ref[p].astype(F32)
    acc[...] = jnp.zeros_like(acc)
    loop()
    for r in range(ice):
        a = acc[r]
        out_ref[0, r : r + 1, :] = 0.5 * (-0.05 * a[1:2] - a[0:1])
        out_ref[1, r : r + 1, :] = a[2:3]
        out_ref[2, r : r + 1, :] = a[3:4]


def forward(code, surf, weights, ice):
    entries = weights.shape[0]
    planes, nbl = surf.shape[:2]
    return pl.pallas_call(
        forward_kernel,
        in_specs=[SM, VM, ANY],
        out_specs=[VM, SM],
        out_shape=[
            jax.ShapeDtypeStruct((3, ice, BS), F32),
            jax.ShapeDtypeStruct((entries + UNROLL + 8,), jnp.int32),
        ],
        scratch_shapes=[
            pltpu.VMEM((planes * nbl, BS), F32),
            pltpu.VMEM((ice, 4, BS), F32),
            pltpu.VMEM((FWD_SLOTS, BS, BS), BF16),
            pltpu.SemaphoreType.DMA((FWD_SLOTS,)),
        ],
        compiler_params=params(),
        name="forward",
    )(code, surf, weights)


def combine_kernel(*refs):
    parts = refs[:-6]
    u_ref, wind_ref, rate_ref, strength_ref, x_ref, rem_ref = refs[-6:]
    vals = [p[...] for p in parts]
    while len(vals) > 1:
        vals = [a + b for a, b in zip(vals[0::2], vals[1::2])]
    rem_ref[...] = vals[0]
    ice = rate_ref.shape[0]
    for r in range(ice):
        for c in range(2):
            u = u_ref[c : c + 1, r * BS : (r + 1) * BS]
            x_ref[2 + c, r : r + 1, :] = u
            x_ref[c, r : r + 1, :] = wind_ref[c : c + 1, r * BS : (r + 1) * BS]
    rate = rate_ref[...]
    for c in range(2):
        x_ref[c] = rate * x_ref[2 + c] + x_ref[c] + rem_ref[1 + c]
    x_ref[4] = rate
    x_ref[5] = strength_ref[...]


def combine(parts, u, wind, rate, strength):
    ice = rate.shape[0]
    return pl.pallas_call(
        combine_kernel,
        in_specs=[VM] * (len(parts) + 4),
        out_specs=[VM, VM],
        out_shape=[
            jax.ShapeDtypeStruct((6, ice, BS), F32),
            jax.ShapeDtypeStruct((3, ice, BS), F32),
        ],
        name="combine",
    )(*parts, u, wind, rate, strength)


def solve_kernel(dst_ref, list_ref, me_ref, x_ref, rem_ref, w_hbm, *refs):
    groups_n, _, ice, _ = x_ref.shape
    outs = refs[:groups_n]
    ice_ref, fin, flux, back, buf, sems = refs[groups_n:]
    entries = dst_ref.shape[0]
    per_block = entries // ice
    nbl = outs[0].shape[1]
    count = list_ref[entries + UNROLL]
    groups = lax.div(count + UNROLL - 1, UNROLL)

    def compute(base, slot):
        for q in range(UNROLL):
            e = list_ref[base + q]
            s = jnp.where(base + q < count, flux[lax.div(e, per_block)], 0.0).astype(BF16)
            part = lax.dot_general(
                s, buf[slot + q], (((1,), (0,)), ((), ())), preferred_element_type=F32
            )
            at = dst_ref[e]
            for f in range(3):
                back[f, pl.ds(at, 1), :] = back[f, pl.ds(at, 1), :] + part[f : f + 1]

    start, loop = stream_weights(list_ref, groups, w_hbm, buf, sems, compute)
    start()
    back[...] = jnp.zeros_like(back)

    n_rows = groups_n * ice
    total = 2.0 * n_rows * BS

    def plane(c):
        return jnp.concatenate([x_ref[a, c] for a in range(groups_n)], axis=0)

    base = [plane(0), plane(1)]
    current = [plane(2), plane(3)]
    rate1 = plane(4) + 1.0
    half_strength = 0.5 * plane(5)
    lane = lax.broadcasted_iota(jnp.int32, (n_rows, BS), 1)
    row = lax.broadcasted_iota(jnp.int32, (n_rows, BS), 0)

    def picard(u):
        left, right = [], []
        for z in u:
            a = pltpu.roll(z, 1, 1)
            b = pltpu.roll(a, 1, 0)
            b = jnp.where(row == 0, 0.0, b)
            left.append(jnp.where(lane == 0, b, a))
            a = pltpu.roll(z, BS - 1, 1)
            b = pltpu.roll(a, n_rows - 1, 0)
            b = jnp.where(row == n_rows - 1, 0.0, b)
            right.append(jnp.where(lane == BS - 1, b, a))
        sx = 0.5 * (right[0] - left[0])
        sy = 0.5 * (right[1] - left[1])
        zeta = half_strength / jnp.sqrt(sx * sx + sy * sy + 0.25)
        den = 1.0 / (rate1 + 2.0 * zeta)
        return [(base[c] + zeta * (left[c] + right[c])) * den for c in range(2)]

    def dot(a, b):
        return jnp.sum(a[0] * b[0] + a[1] * b[1], keepdims=True) / total

    gvals, fvals, df, dg, gram, norms = [], [], [], [], {}, []
    for step in range(ITERS):
        gnew = picard(current)
        f = [gnew[c] - current[c] for c in range(2)]
        if step == 0:
            gvals, fvals = gnew, f
            current = gnew
            continue
        df.append([f[c] - fvals[c] for c in range(2)])
        dg.append([gnew[c] - gvals[c] for c in range(2)])
        gvals, fvals = gnew, f
        j = step - 1
        for i in range(j + 1):
            gram[i, j] = dot(df[i], df[j])
        norms.append(jnp.sqrt(gram[j, j] + 1e-06))
        used = list(range(max(0, step - DEPTH), step))
        m = len(used)
        a = [[None] * m for _ in range(m)]
        for p in range(m):
            for q in range(p + 1):
                i, k = used[q], used[p]
                a[p][q] = gram[i, k] / (norms[i] * norms[k])
            a[p][p] = a[p][p] + 0.1
        h = [dot(df[i], f) / norms[i] for i in used]
        d = [None] * m
        low = [[None] * m for _ in range(m)]
        y = [None] * m
        for p in range(m):
            acc = h[p]
            for q in range(p):
                v = a[p][q]
                for s in range(q):
                    v = v - low[p][s] * low[q][s] * d[s]
                low[p][q] = v / d[q]
                acc = acc - low[p][q] * y[q]
            v = a[p][p]
            for s in range(p):
                v = v - low[p][s] * low[p][s] * d[s]
            d[p] = v
            y[p] = acc
        coef = [None] * m
        for p in reversed(range(m)):
            v = y[p] / d[p]
            for q in range(p + 1, m):
                v = v - low[q][p] * coef[q]
            coef[p] = v
        current = list(gnew)
        for p, i in enumerate(used):
            scale = coef[p] / norms[i]
            for c in range(2):
                current[c] = current[c] - scale * dg[i][c]
    fin[0] = current[0]
    fin[1] = current[1]
    mine = pl.multiple_of(me_ref[0] * ice, ice)
    own = [fin[c, pl.ds(mine, ice), :] for c in range(2)]
    planes = [own[0] - rem_ref[1], own[1] - rem_ref[2], rem_ref[0]]
    for r in range(ice):
        for c in range(2):
            ice_ref[c : c + 1, r * BS : (r + 1) * BS] = own[c][r : r + 1]
        for f in range(3):
            flux[r, f : f + 1, :] = planes[f][r : r + 1]
        flux[r, 3:4, :] = jnp.zeros((1, BS), F32)
    loop()
    for k in range(groups_n):
        outs[k][...] = back[:, k * nbl : (k + 1) * nbl, :]


def solve(dst, lst, me, x, rem, weights, nbl):
    groups_n, _, ice, _ = x.shape
    chunk = jax.ShapeDtypeStruct((3, nbl, BS), F32)
    return pl.pallas_call(
        solve_kernel,
        in_specs=[SM, SM, SM, VM, VM, ANY],
        out_specs=[VM] * (groups_n + 1),
        out_shape=[chunk] * groups_n + [jax.ShapeDtypeStruct((2, ice * BS), F32)],
        scratch_shapes=[
            pltpu.VMEM((2, groups_n * ice, BS), F32),
            pltpu.VMEM((ice, 4, BS), F32),
            pltpu.VMEM((3, groups_n * nbl, BS), F32),
            pltpu.VMEM((BWD_SLOTS, BS, BS), BF16),
            pltpu.SemaphoreType.DMA((BWD_SLOTS,)),
        ],
        compiler_params=params(),
        name="solve",
    )(dst, lst, me, x, rem, weights)


def finish_kernel(*refs):
    chunks = refs[:-3]
    t_ref, flux_ref, out_ref = refs[-3:]
    height, across = t_ref.shape[2:]
    for f in range(3):
        for h in range(across // BS):
            v = chunks[0][f, h * height : (h + 1) * height, :]
            for c in chunks[1:]:
                v = v + c[f, h * height : (h + 1) * height, :]
            flux_ref[f, :, h * BS : (h + 1) * BS] = v
    out_ref[0, 0] = t_ref[0, 0] + 0.5 * flux_ref[2]


def finish(chunks, tracers_next):
    height, across = tracers_next.shape[2:]
    whole = pl.BlockSpec(chunks[0].shape, lambda i: (0, 0, 0))
    level = pl.BlockSpec((1, 1, height, across), lambda i: (0, 0, 0, 0))
    return pl.pallas_call(
        finish_kernel,
        grid=(1,),
        in_specs=[whole] * len(chunks) + [level],
        out_specs=[pl.BlockSpec((3, height, across), lambda i: (0, 0, 0)), level],
        out_shape=[
            jax.ShapeDtypeStruct((3, height, across), F32),
            jax.ShapeDtypeStruct(tracers_next.shape, F32),
        ],
        input_output_aliases={len(chunks): 1},
        name="finish",
    )(*chunks, tracers_next)


def neighbours(low_edge, high_edge, axis):
    n = lax.axis_size(axis)
    up = [(i, i + 1) for i in range(n - 1)]
    down = [(i + 1, i) for i in range(n - 1)]
    return lax.ppermute(high_edge, axis, up), lax.ppermute(low_edge, axis, down)


def on_device(
    tracers,
    velocity,
    remap_weights,
    remap_blocks,
    remap_count,
    ice_velocity,
    ice_mass_rate,
    ice_strength,
    wind_stress,
):
    n_grp = lax.axis_size("grp")
    n_ocn = lax.axis_size("ocn")
    column = lax.axis_index("ocn")
    me = lax.axis_index("grp")
    height, across = tracers.shape[2:]
    halves = across // BS
    nbl = height * halves
    ice, per_block = remap_blocks.shape
    weights = remap_weights.reshape(ice * per_block, BS, BS)

    local = remap_blocks % (n_grp * nbl)
    tile = local // nbl
    j = local % nbl
    place = (j % halves) * height + j // halves
    mine = (jnp.arange(per_block)[None, :] < remap_count[:, None]) & (
        remap_blocks // (n_grp * nbl) == column
    )
    code = jnp.where(mine, tile * (4 * nbl) + place, -1).reshape(-1)
    dst = (((tile - me) % n_grp) * nbl + place).reshape(-1)

    row0, rown, col0, coln = pack_edges(tracers)
    south, north = neighbours(row0, rown, "grp")
    west, east = neighbours(col0, coln, "ocn")

    surf = lax.all_gather(pack_surface(tracers, velocity), "grp", axis=0, tiled=True)
    part, lst = forward(code, surf, weights, ice)
    if n_ocn & (n_ocn - 1) == 0:
        parts = [part]
        for k in range(1, n_ocn):
            parts.append(lax.ppermute(part, "ocn", [(i, i ^ k) for i in range(n_ocn)]))
    else:
        parts = [lax.psum(part, "ocn")]
    x, rem = combine(
        parts,
        ice_velocity,
        wind_stress,
        ice_mass_rate.reshape(ice, BS),
        ice_strength.reshape(ice, BS),
    )
    xg = lax.all_gather(x, "grp", axis=0)
    *chunks, ice_final = solve(dst, lst, me.reshape(1), xg, rem, weights, nbl)
    moved = [chunks[0]]
    for k in range(1, n_grp):
        moved.append(lax.ppermute(chunks[k], "grp", [(i, (i + k) % n_grp) for i in range(n_grp)]))
    tracers_next = stencil(tracers, velocity, north, south, east, west)
    surface_flux, tracers_next = finish(moved, tracers_next)
    return tracers_next, surface_flux, ice_final


def solution(mesh):
    return jax.shard_map(
        on_device,
        mesh=mesh,
        in_specs=(
            P(None, None, "grp", "ocn"),
            P(None, None, "grp", "ocn"),
            P("grp", None, None, None),
            P("grp", None),
            P("grp"),
            P(None, "grp"),
            P("grp"),
            P("grp"),
            P(None, "grp"),
        ),
        out_specs=(P(None, None, "grp", "ocn"), P(None, "grp", "ocn"), P(None, "grp")),
        check_vma=False,
    )
```

```python
import jax
import jax.numpy as jnp
from jax import lax
from jax.experimental import pallas as pl
from jax.experimental.pallas import tpu as pltpu
from jax.sharding import PartitionSpec as P


BS = 128
ITERS = 4
DEPTH = 3
UNROLL = 8
FWD_SLOTS = 32
BWD_SLOTS = 64
F32 = jnp.float32
BF16 = jnp.bfloat16


VM = pl.BlockSpec(memory_space=pltpu.VMEM)
SM = pl.BlockSpec(memory_space=pltpu.SMEM)
ANY = pl.BlockSpec(memory_space=pl.ANY)


def params(**kw):
    return pltpu.CompilerParams(vmem_limit_bytes=48 * 1024 * 1024, **kw)


def surface_kernel(t_ref, v_ref, out_ref):
    height, across = t_ref.shape[2], t_ref.shape[3]
    for f in range(4):
        src = t_ref if f < 2 else v_ref
        for h in range(across // BS):
            out_ref[f, h * height : (h + 1) * height, :] = src[
                f % 2, 0, :, h * BS : (h + 1) * BS
            ].astype(BF16)


def pack_surface(tracers, velocity):
    height, across = tracers.shape[2:]
    spec = pl.BlockSpec((2, 1, height, across), lambda i: (0, 0, 0, 0))
    nbl = height * across // BS
    return pl.pallas_call(
        surface_kernel,
        grid=(1,),
        in_specs=[spec, spec],
        out_specs=pl.BlockSpec((4, nbl, BS), lambda i: (0, 0, 0)),
        out_shape=jax.ShapeDtypeStruct((4, nbl, BS), BF16),
        name="surface",
    )(tracers, velocity)


def edges_kernel(t_ref, row0_ref, rown_ref, col0_ref, coln_ref):
    step = pl.program_id(0)
    lc, height, across = t_ref.shape[1:]
    levels = lc * pl.num_programs(0)
    lane = lax.broadcasted_iota(jnp.int32, (height, BS), 1)

    @pl.when(step == 0)
    def _():
        col0_ref[...] = jnp.zeros_like(col0_ref)
        coln_ref[...] = jnp.zeros_like(coln_ref)

    first = col0_ref[...]
    last = coln_ref[...]
    for t in range(2):
        for i in range(lc):
            c = t * levels + step * lc + i
            first = jnp.where(lane == c, pltpu.roll(t_ref[t, i, :, :BS], c, 1), first)
            last = jnp.where(
                lane == c, pltpu.roll(t_ref[t, i, :, across - BS :], (c + 1) % BS, 1), last
            )
            row0_ref[t, i : i + 1, :] = t_ref[t, i, 0:1, :]
            rown_ref[t, i : i + 1, :] = t_ref[t, i, height - 1 : height, :]
    col0_ref[...] = first
    coln_ref[...] = last


def pack_edges(tracers):
    _, levels, height, across = tracers.shape
    lc = 8
    rows = jax.ShapeDtypeStruct((2, levels, across), F32)
    cols = jax.ShapeDtypeStruct((height, BS), F32)
    row_spec = pl.BlockSpec((2, lc, across), lambda i: (0, i, 0))
    col_spec = pl.BlockSpec((height, BS), lambda i: (0, 0))
    return pl.pallas_call(
        edges_kernel,
        grid=(levels // lc,),
        in_specs=[pl.BlockSpec((2, lc, height, across), lambda i: (0, i, 0, 0))],
        out_specs=[row_spec, row_spec, col_spec, col_spec],
        out_shape=[rows, rows, cols, cols],
        name="edges",
    )(tracers)


def stencil_kernel(t_ref, up_ref, dn_ref, v_ref, north_ref, south_ref, east_ref, west_ref, out_ref):
    step = pl.program_id(0)
    steps = pl.num_programs(0)
    lc, height, across = t_ref.shape[1:]
    levels = lc * steps
    lane = lax.broadcasted_iota(jnp.int32, (height, across), 1)
    row = lax.broadcasted_iota(jnp.int32, (height, across), 0)
    pad = jnp.zeros((height, across - BS), F32)
    top = jnp.where(step == 0, 0.0, 1.0)
    bottom = jnp.where(step == steps - 1, 0.0, 1.0)
    for i in range(lc):
        u = v_ref[0, i]
        v = v_ref[1, i]
        for t in range(2):
            c = t * levels + step * lc + i
            x = t_ref[t, i]
            above = up_ref[t, 0] * top if i == 0 else t_ref[t, i - 1]
            below = dn_ref[t, 0] * bottom if i == lc - 1 else t_ref[t, i + 1]
            wcol = jnp.concatenate(
                [pltpu.roll(west_ref[...], (BS - c) % BS, 1), pad], axis=1
            )
            ecol = jnp.concatenate([pad, pltpu.roll(east_ref[...], BS - 1 - c, 1)], axis=1)
            w = jnp.where(lane == 0, wcol, pltpu.roll(x, 1, 1))
            e = jnp.where(lane == across - 1, ecol, pltpu.roll(x, across - 1, 1))
            s = jnp.where(row == 0, south_ref[t, i : i + 1, :], pltpu.roll(x, 1, 0))
            n = jnp.where(row == height - 1, north_ref[t, i : i + 1, :], pltpu.roll(x, height - 1, 0))
            advect = u * (e - w) * 0.5 + v * (n - s) * 0.5
            out_ref[t, i] = (
                x
                + 0.2 * (e + w + n + s - 4.0 * x)
                - 0.5 * advect
                + 0.2 * (above + below - 2.0 * x)
            )


def stencil(tracers, velocity, north, south, east, west):
    _, levels, height, across = tracers.shape
    lc = 8
    main = pl.BlockSpec((2, lc, height, across), lambda i: (0, i, 0, 0))
    up = pl.BlockSpec((2, 1, height, across), lambda i: (0, jnp.maximum(i * lc - 1, 0), 0, 0))
    dn = pl.BlockSpec(
        (2, 1, height, across), lambda i: (0, jnp.minimum(i * lc + lc, levels - 1), 0, 0)
    )
    row_spec = pl.BlockSpec((2, lc, across), lambda i: (0, i, 0))
    col_spec = pl.BlockSpec((height, BS), lambda i: (0, 0))
    return pl.pallas_call(
        stencil_kernel,
        grid=(levels // lc,),
        in_specs=[main, up, dn, main, row_spec, row_spec, col_spec, col_spec],
        out_specs=main,
        out_shape=jax.ShapeDtypeStruct(tracers.shape, F32),
        cost_estimate=pl.CostEstimate(
            flops=120_000_000, bytes_accessed=4 * tracers.size * 4, transcendentals=0
        ),
        name="stencil",
    )(tracers, tracers, tracers, velocity, north, south, east, west)


def stream_weights(list_ref, groups, w_hbm, buf, sems, compute):
    slots = buf.shape[0]

    def copy(i, slot):
        return pltpu.make_async_copy(w_hbm.at[list_ref[i]], buf.at[slot], sems.at[slot])

    def start():
        for s in range(slots // UNROLL):

            @pl.when(s < groups)
            def _():
                for q in range(UNROLL):
                    copy(s * UNROLL + q, s * UNROLL + q).start()

    def loop():
        def body(g, carry):
            base = g * UNROLL
            slot = lax.rem(g, slots // UNROLL) * UNROLL
            for q in range(UNROLL):
                copy(base + q, slot + q).wait()
            compute(base, slot)

            @pl.when(g + slots // UNROLL < groups)
            def _():
                for q in range(UNROLL):
                    copy(base + slots + q, slot + q).start()

            return carry

        lax.fori_loop(0, groups, body, 0)

    return start, loop


def forward_kernel(code_ref, surf_ref, w_hbm, out_ref, list_ref, rows, acc, buf, sems):
    entries = code_ref.shape[0]
    ice = acc.shape[0]
    per_block = entries // ice
    nbl = surf_ref.shape[1]

    def scan(i, n):
        for q in range(8):
            e = i * 8 + q
            list_ref[n] = e
            n = n + jnp.where(code_ref[e] >= 0, 1, 0)
        return n

    count = lax.fori_loop(0, entries // 8, scan, 0)
    for q in range(UNROLL):
        list_ref[count + q] = 0
    list_ref[entries + UNROLL] = count
    groups = lax.div(count + UNROLL - 1, UNROLL)
    first = lax.broadcasted_iota(jnp.int32, (4, BS), 0)

    def compute(base, slot):
        for q in range(UNROLL):
            e = list_ref[base + q]
            at = jnp.maximum(code_ref[e], 0)
            r0 = jnp.broadcast_to(rows[pl.ds(at, 1), :], (4, BS))
            r1 = jnp.broadcast_to(rows[pl.ds(at + nbl, 1), :], (4, BS))
            r2 = jnp.broadcast_to(rows[pl.ds(at + 2 * nbl, 1), :], (4, BS))
            r3 = jnp.broadcast_to(rows[pl.ds(at + 3 * nbl, 1), :], (4, BS))
            s = jnp.where(first == 0, r0, jnp.where(first == 1, r1, jnp.where(first == 2, r2, r3)))
            s = jnp.where(base + q < count, s, 0.0).astype(BF16)
            part = lax.dot_general(
                s, buf[slot + q], (((1,), (1,)), ((), ())), preferred_element_type=F32
            )
            r = lax.div(e, per_block)
            acc[r] = acc[r] + part

    start, loop = stream_weights(list_ref, groups, w_hbm, buf, sems, compute)
    start()
    planes = surf_ref.shape[0]
    for p in range(planes):
        rows[p * nbl : (p + 1) * nbl, :] = surf_ref[p].astype(F32)
    acc[...] = jnp.zeros_like(acc)
    loop()
    for r in range(ice):
        a = acc[r]
        out_ref[0, r : r + 1, :] = 0.5 * (-0.05 * a[1:2] - a[0:1])
        out_ref[1, r : r + 1, :] = a[2:3]
        out_ref[2, r : r + 1, :] = a[3:4]


def forward(code, surf, weights, ice):
    entries = weights.shape[0]
    planes, nbl = surf.shape[:2]
    return pl.pallas_call(
        forward_kernel,
        in_specs=[SM, VM, ANY],
        out_specs=[VM, SM],
        out_shape=[
            jax.ShapeDtypeStruct((3, ice, BS), F32),
            jax.ShapeDtypeStruct((entries + UNROLL + 8,), jnp.int32),
        ],
        scratch_shapes=[
            pltpu.VMEM((planes * nbl, BS), F32),
            pltpu.VMEM((ice, 4, BS), F32),
            pltpu.VMEM((FWD_SLOTS, BS, BS), BF16),
            pltpu.SemaphoreType.DMA((FWD_SLOTS,)),
        ],
        compiler_params=params(),
        name="forward",
    )(code, surf, weights)


def combine_kernel(*refs):
    parts = refs[:-6]
    u_ref, wind_ref, rate_ref, strength_ref, x_ref, rem_ref = refs[-6:]
    vals = [p[...] for p in parts]
    while len(vals) > 1:
        vals = [a + b for a, b in zip(vals[0::2], vals[1::2])]
    rem_ref[...] = vals[0]
    ice = rate_ref.shape[0]
    for r in range(ice):
        for c in range(2):
            u = u_ref[c : c + 1, r * BS : (r + 1) * BS]
            x_ref[2 + c, r : r + 1, :] = u
            x_ref[c, r : r + 1, :] = wind_ref[c : c + 1, r * BS : (r + 1) * BS]
    rate = rate_ref[...]
    for c in range(2):
        x_ref[c] = rate * x_ref[2 + c] + x_ref[c] + rem_ref[1 + c]
    x_ref[4] = rate
    x_ref[5] = strength_ref[...]


def combine(parts, u, wind, rate, strength):
    ice = rate.shape[0]
    return pl.pallas_call(
        combine_kernel,
        in_specs=[VM] * (len(parts) + 4),
        out_specs=[VM, VM],
        out_shape=[
            jax.ShapeDtypeStruct((6, ice, BS), F32),
            jax.ShapeDtypeStruct((3, ice, BS), F32),
        ],
        name="combine",
    )(*parts, u, wind, rate, strength)


def solve_kernel(dst_ref, list_ref, me_ref, x_ref, rem_ref, w_hbm, *refs):
    groups_n, _, ice, _ = x_ref.shape
    outs = refs[:groups_n]
    ice_ref, fin, flux, back, buf, sems = refs[groups_n:]
    entries = dst_ref.shape[0]
    per_block = entries // ice
    nbl = outs[0].shape[1]
    count = list_ref[entries + UNROLL]
    groups = lax.div(count + UNROLL - 1, UNROLL)

    def compute(base, slot):
        for q in range(UNROLL):
            e = list_ref[base + q]
            s = jnp.where(base + q < count, flux[lax.div(e, per_block)], 0.0).astype(BF16)
            part = lax.dot_general(
                s, buf[slot + q], (((1,), (0,)), ((), ())), preferred_element_type=F32
            )
            at = dst_ref[e]
            for f in range(3):
                back[f, pl.ds(at, 1), :] = back[f, pl.ds(at, 1), :] + part[f : f + 1]

    start, loop = stream_weights(list_ref, groups, w_hbm, buf, sems, compute)
    start()
    back[...] = jnp.zeros_like(back)

    n_rows = groups_n * ice
    total = 2.0 * n_rows * BS

    def plane(c):
        return jnp.concatenate([x_ref[a, c] for a in range(groups_n)], axis=0)

    base = [plane(0), plane(1)]
    current = [plane(2), plane(3)]
    rate1 = plane(4) + 1.0
    half_strength = 0.5 * plane(5)
    lane = lax.broadcasted_iota(jnp.int32, (n_rows, BS), 1)
    row = lax.broadcasted_iota(jnp.int32, (n_rows, BS), 0)

    def picard(u):
        left, right = [], []
        for z in u:
            a = pltpu.roll(z, 1, 1)
            b = pltpu.roll(a, 1, 0)
            b = jnp.where(row == 0, 0.0, b)
            left.append(jnp.where(lane == 0, b, a))
            a = pltpu.roll(z, BS - 1, 1)
            b = pltpu.roll(a, n_rows - 1, 0)
            b = jnp.where(row == n_rows - 1, 0.0, b)
            right.append(jnp.where(lane == BS - 1, b, a))
        sx = 0.5 * (right[0] - left[0])
        sy = 0.5 * (right[1] - left[1])
        zeta = half_strength / jnp.sqrt(sx * sx + sy * sy + 0.25)
        den = 1.0 / (rate1 + 2.0 * zeta)
        return [(base[c] + zeta * (left[c] + right[c])) * den for c in range(2)]

    def dot(a, b):
        return jnp.sum(a[0] * b[0] + a[1] * b[1], keepdims=True) / total

    gvals, fvals, df, dg, gram, norms = [], [], [], [], {}, []
    for step in range(ITERS):
        gnew = picard(current)
        f = [gnew[c] - current[c] for c in range(2)]
        if step == 0:
            gvals, fvals = gnew, f
            current = gnew
            continue
        df.append([f[c] - fvals[c] for c in range(2)])
        dg.append([gnew[c] - gvals[c] for c in range(2)])
        gvals, fvals = gnew, f
        j = step - 1
        for i in range(j + 1):
            gram[i, j] = dot(df[i], df[j])
        norms.append(jnp.sqrt(gram[j, j] + 1e-06))
        used = list(range(max(0, step - DEPTH), step))
        m = len(used)
        a = [[None] * m for _ in range(m)]
        for p in range(m):
            for q in range(p + 1):
                i, k = used[q], used[p]
                a[p][q] = gram[i, k] / (norms[i] * norms[k])
            a[p][p] = a[p][p] + 0.1
        h = [dot(df[i], f) / norms[i] for i in used]
        d = [None] * m
        low = [[None] * m for _ in range(m)]
        y = [None] * m
        for p in range(m):
            acc = h[p]
            for q in range(p):
                v = a[p][q]
                for s in range(q):
                    v = v - low[p][s] * low[q][s] * d[s]
                low[p][q] = v / d[q]
                acc = acc - low[p][q] * y[q]
            v = a[p][p]
            for s in range(p):
                v = v - low[p][s] * low[p][s] * d[s]
            d[p] = v
            y[p] = acc
        coef = [None] * m
        for p in reversed(range(m)):
            v = y[p] / d[p]
            for q in range(p + 1, m):
                v = v - low[q][p] * coef[q]
            coef[p] = v
        current = list(gnew)
        for p, i in enumerate(used):
            scale = coef[p] / norms[i]
            for c in range(2):
                current[c] = current[c] - scale * dg[i][c]
    fin[0] = current[0]
    fin[1] = current[1]
    mine = pl.multiple_of(me_ref[0] * ice, ice)
    own = [fin[c, pl.ds(mine, ice), :] for c in range(2)]
    planes = [own[0] - rem_ref[1], own[1] - rem_ref[2], rem_ref[0]]
    for r in range(ice):
        for c in range(2):
            ice_ref[c : c + 1, r * BS : (r + 1) * BS] = own[c][r : r + 1]
        for f in range(3):
            flux[r, f : f + 1, :] = planes[f][r : r + 1]
        flux[r, 3:4, :] = jnp.zeros((1, BS), F32)
    loop()
    for k in range(groups_n):
        outs[k][...] = back[:, k * nbl : (k + 1) * nbl, :]


def solve(dst, lst, me, x, rem, weights, nbl):
    groups_n, _, ice, _ = x.shape
    chunk = jax.ShapeDtypeStruct((3, nbl, BS), F32)
    return pl.pallas_call(
        solve_kernel,
        in_specs=[SM, SM, SM, VM, VM, ANY],
        out_specs=[VM] * (groups_n + 1),
        out_shape=[chunk] * groups_n + [jax.ShapeDtypeStruct((2, ice * BS), F32)],
        scratch_shapes=[
            pltpu.VMEM((2, groups_n * ice, BS), F32),
            pltpu.VMEM((ice, 4, BS), F32),
            pltpu.VMEM((3, groups_n * nbl, BS), F32),
            pltpu.VMEM((BWD_SLOTS, BS, BS), BF16),
            pltpu.SemaphoreType.DMA((BWD_SLOTS,)),
        ],
        compiler_params=params(),
        name="solve",
    )(dst, lst, me, x, rem, weights)


def finish_kernel(*refs):
    chunks = refs[:-3]
    t_ref, flux_ref, out_ref = refs[-3:]
    height, across = t_ref.shape[2:]
    for f in range(3):
        for h in range(across // BS):
            v = chunks[0][f, h * height : (h + 1) * height, :]
            for c in chunks[1:]:
                v = v + c[f, h * height : (h + 1) * height, :]
            flux_ref[f, :, h * BS : (h + 1) * BS] = v
    out_ref[0, 0] = t_ref[0, 0] + 0.5 * flux_ref[2]


def finish(chunks, tracers_next):
    height, across = tracers_next.shape[2:]
    whole = pl.BlockSpec(chunks[0].shape, lambda i: (0, 0, 0))
    level = pl.BlockSpec((1, 1, height, across), lambda i: (0, 0, 0, 0))
    return pl.pallas_call(
        finish_kernel,
        grid=(1,),
        in_specs=[whole] * len(chunks) + [level],
        out_specs=[pl.BlockSpec((3, height, across), lambda i: (0, 0, 0)), level],
        out_shape=[
            jax.ShapeDtypeStruct((3, height, across), F32),
            jax.ShapeDtypeStruct(tracers_next.shape, F32),
        ],
        input_output_aliases={len(chunks): 1},
        name="finish",
    )(*chunks, tracers_next)


def neighbours(low_edge, high_edge, axis):
    n = lax.axis_size(axis)
    up = [(i, i + 1) for i in range(n - 1)]
    down = [(i + 1, i) for i in range(n - 1)]
    return lax.ppermute(high_edge, axis, up), lax.ppermute(low_edge, axis, down)


def coupled_step(
    tracers,
    velocity,
    remap_weights,
    remap_blocks,
    remap_count,
    ice_velocity,
    ice_mass_rate,
    ice_strength,
    wind_stress,
):
    n_grp = lax.axis_size("grp")
    n_ocn = lax.axis_size("ocn")
    column = lax.axis_index("ocn")
    me = lax.axis_index("grp")
    height, across = tracers.shape[2:]
    halves = across // BS
    nbl = height * halves
    ice, per_block = remap_blocks.shape
    weights = remap_weights.reshape(ice * per_block, BS, BS)

    local = remap_blocks % (n_grp * nbl)
    tile = local // nbl
    j = local % nbl
    place = (j % halves) * height + j // halves
    mine = (jnp.arange(per_block)[None, :] < remap_count[:, None]) & (
        remap_blocks // (n_grp * nbl) == column
    )
    code = jnp.where(mine, tile * (4 * nbl) + place, -1).reshape(-1)
    dst = (((tile - me) % n_grp) * nbl + place).reshape(-1)

    row0, rown, col0, coln = pack_edges(tracers)
    south, north = neighbours(row0, rown, "grp")
    west, east = neighbours(col0, coln, "ocn")

    surf = lax.all_gather(pack_surface(tracers, velocity), "grp", axis=0, tiled=True)
    part, lst = forward(code, surf, weights, ice)
    if n_ocn & (n_ocn - 1) == 0:
        parts = [part]
        for k in range(1, n_ocn):
            parts.append(lax.ppermute(part, "ocn", [(i, i ^ k) for i in range(n_ocn)]))
    else:
        parts = [lax.psum(part, "ocn")]
    x, rem = combine(
        parts,
        ice_velocity,
        wind_stress,
        ice_mass_rate.reshape(ice, BS),
        ice_strength.reshape(ice, BS),
    )
    xg = lax.all_gather(x, "grp", axis=0)
    *chunks, ice_final = solve(dst, lst, me.reshape(1), xg, rem, weights, nbl)
    moved = [chunks[0]]
    for k in range(1, n_grp):
        ring = [(i, (i + k) % n_grp) for i in range(n_grp)]
        moved.append(lax.ppermute(chunks[k], "grp", ring))
    tracers_next = stencil(tracers, velocity, north, south, east, west)
    surface_flux, tracers_next = finish(moved, tracers_next)
    return tracers_next, surface_flux, ice_final


def solution(mesh):
    return jax.shard_map(
        coupled_step,
        mesh=mesh,
        in_specs=(
            P(None, None, "grp", "ocn"),
            P(None, None, "grp", "ocn"),
            P("grp", None, None, None),
            P("grp", None),
            P("grp"),
            P(None, "grp"),
            P("grp"),
            P("grp"),
            P(None, "grp"),
        ),
        out_specs=(P(None, None, "grp", "ocn"), P(None, "grp", "ocn"), P(None, "grp")),
        check_vma=False,
    )
```

```python
import functools

import jax
import jax.numpy as jnp
from jax import lax
from jax.experimental import pallas as pl
from jax.experimental.pallas import tpu as pltpu
from jax.sharding import PartitionSpec as P


BS = 128
ITERS = 4
DEPTH = 3
UNROLL = 8
FWD_SLOTS = 32
BWD_SLOTS = 64
F32 = jnp.float32
BF16 = jnp.bfloat16


VM = pl.BlockSpec(memory_space=pltpu.VMEM)
SM = pl.BlockSpec(memory_space=pltpu.SMEM)
ANY = pl.BlockSpec(memory_space=pltpu.HBM)


def in_hbm(x):
    return pltpu.with_memory_space_constraint(x, pltpu.HBM)


def params(mib):
    return pltpu.CompilerParams(vmem_limit_bytes=mib * 1024 * 1024)


def surface_kernel(code_ref, t_hbm, v_hbm, out_ref, list_ref, buf, sems):
    height, across = buf.shape[1:]
    entries = code_ref.shape[0]
    copies = [
        pltpu.make_async_copy(
            (t_hbm if f < 2 else v_hbm).at[f % 2, 0], buf.at[f], sems.at[f]
        )
        for f in range(4)
    ]
    for c in copies:
        c.start()

    def scan(i, n):
        for q in range(8):
            e = i * 8 + q
            list_ref[n] = e
            n = n + jnp.where(code_ref[e] >= 0, 1, 0)
        return n

    count = lax.fori_loop(0, entries // 8, scan, 0)
    for q in range(UNROLL):
        list_ref[count + q] = 0
    list_ref[entries + UNROLL] = count
    for c in copies:
        c.wait()
    for f in range(4):
        for h in range(across // BS):
            out_ref[f, h * height : (h + 1) * height, :] = buf[
                f, :, h * BS : (h + 1) * BS
            ].astype(BF16)


def pack_surface(code, tracers, velocity):
    height, across = tracers.shape[2:]
    nbl = height * across // BS
    return pl.pallas_call(
        surface_kernel,
        in_specs=[SM, ANY, ANY],
        out_specs=[VM, SM],
        out_shape=[
            jax.ShapeDtypeStruct((4, nbl, BS), BF16),
            jax.ShapeDtypeStruct((code.shape[0] + UNROLL + 8,), jnp.int32),
        ],
        scratch_shapes=[
            pltpu.VMEM((4, height, across), F32),
            pltpu.SemaphoreType.DMA((4,)),
        ],
        compiler_params=params(4),
        name="surface",
    )(code, in_hbm(tracers), in_hbm(velocity))


def stencil_kernel(
    n_grp, me_ref, t_ref, up_ref, dn_ref, v_ref, south_ref, north_ref, cols_ref, out_ref
):
    step = pl.program_id(0)
    steps = pl.num_programs(0)
    lc, height, across = t_ref.shape[1:]
    halves = across // BS
    levels = lc * steps
    skip = south_ref.shape[0] - 2 * levels * halves
    lane = lax.broadcasted_iota(jnp.int32, (height, across), 1)
    row = lax.broadcasted_iota(jnp.int32, (height, across), 0)
    pad = jnp.zeros((height, across - BS), F32)
    top = jnp.where(step == 0, 0.0, 1.0)
    bottom = jnp.where(step == steps - 1, 0.0, 1.0)
    no_south = jnp.where(me_ref[0] == 0, 0.0, 1.0)
    no_north = jnp.where(me_ref[0] == n_grp - 1, 0.0, 1.0)

    def outer_row(ref, c):
        pieces = [ref[pl.ds(skip + h * 2 * levels + c, 1), :] for h in range(halves)]
        return jnp.concatenate(pieces, axis=1)

    for i in range(lc):
        u = v_ref[0, i]
        v = v_ref[1, i]
        for t in range(2):
            c = t * levels + step * lc + i
            x = t_ref[t, i]
            above = up_ref[t, 0] * top if i == 0 else t_ref[t, i - 1]
            below = dn_ref[t, 0] * bottom if i == lc - 1 else t_ref[t, i + 1]
            cols = cols_ref[...]
            wcol = jnp.concatenate([pltpu.roll(cols, BS // 2 - c, 1), pad], axis=1)
            ecol = jnp.concatenate([pad, pltpu.roll(cols, BS - 1 - c, 1)], axis=1)
            south = outer_row(south_ref, c) * no_south
            north = outer_row(north_ref, c) * no_north
            w = jnp.where(lane == 0, wcol, pltpu.roll(x, 1, 1))
            e = jnp.where(lane == across - 1, ecol, pltpu.roll(x, across - 1, 1))
            s = jnp.where(row == 0, south, pltpu.roll(x, 1, 0))
            n = jnp.where(row == height - 1, north, pltpu.roll(x, height - 1, 0))
            advect = u * (e - w) * 0.5 + v * (n - s) * 0.5
            out_ref[t, i] = (
                x
                + 0.2 * (e + w + n + s - 4.0 * x)
                - 0.5 * advect
                + 0.2 * (above + below - 2.0 * x)
            )


def stencil(me, n_grp, tracers, velocity, south, north, cols):
    _, levels, height, across = tracers.shape
    lc = 8
    main = pl.BlockSpec((2, lc, height, across), lambda i: (0, i, 0, 0))
    up = pl.BlockSpec((2, 1, height, across), lambda i: (0, jnp.maximum(i * lc - 1, 0), 0, 0))
    dn = pl.BlockSpec(
        (2, 1, height, across), lambda i: (0, jnp.minimum(i * lc + lc, levels - 1), 0, 0)
    )
    return pl.pallas_call(
        functools.partial(stencil_kernel, n_grp),
        grid=(levels // lc,),
        in_specs=[SM, main, up, dn, main, VM, VM, VM],
        out_specs=main,
        out_shape=jax.ShapeDtypeStruct(tracers.shape, F32),
        compiler_params=params(14),
        cost_estimate=pl.CostEstimate(
            flops=120_000_000, bytes_accessed=4 * tracers.size * 4, transcendentals=0
        ),
        name="stencil",
    )(me, tracers, tracers, tracers, velocity, south, north, cols)


def stream_weights(list_ref, groups, w_hbm, buf, sems, compute):
    slots = buf.shape[0]

    def copy(i, slot):
        return pltpu.make_async_copy(w_hbm.at[list_ref[i]], buf.at[slot], sems.at[slot])

    def start():
        for s in range(slots // UNROLL):

            @pl.when(s < groups)
            def _():
                for q in range(UNROLL):
                    copy(s * UNROLL + q, s * UNROLL + q).start()

    def loop():
        def body(g, carry):
            base = g * UNROLL
            slot = lax.rem(g, slots // UNROLL) * UNROLL
            for q in range(UNROLL):
                copy(base + q, slot + q).wait()
            compute(base, slot)

            @pl.when(g + slots // UNROLL < groups)
            def _():
                for q in range(UNROLL):
                    copy(base + slots + q, slot + q).start()

            return carry

        lax.fori_loop(0, groups, body, 0)

    return start, loop


def forward_kernel(
    code_ref, list_ref, surf_ref, w_hbm, t_hbm, out_ref, row0_ref, rown_ref, rows, acc, tiles, buf, sems, t_sem
):
    entries = code_ref.shape[0]
    ice = acc.shape[0]
    per_block = entries // ice
    nbl = surf_ref.shape[1]
    count = list_ref[entries + UNROLL]
    groups = lax.div(count + UNROLL - 1, UNROLL)
    first = lax.broadcasted_iota(jnp.int32, (4, BS), 0)

    def compute(base, slot):
        for q in range(UNROLL):
            e = list_ref[base + q]
            at = jnp.maximum(code_ref[e], 0)
            r0 = jnp.broadcast_to(rows[pl.ds(at, 1), :], (4, BS))
            r1 = jnp.broadcast_to(rows[pl.ds(at + nbl, 1), :], (4, BS))
            r2 = jnp.broadcast_to(rows[pl.ds(at + 2 * nbl, 1), :], (4, BS))
            r3 = jnp.broadcast_to(rows[pl.ds(at + 3 * nbl, 1), :], (4, BS))
            s = jnp.where(first == 0, r0, jnp.where(first == 1, r1, jnp.where(first == 2, r2, r3)))
            s = jnp.where(base + q < count, s, 0.0).astype(BF16)
            part = lax.dot_general(
                s, buf[slot + q], (((1,), (1,)), ((), ())), preferred_element_type=F32
            )
            r = lax.div(e, per_block)
            acc[r] = acc[r] + part

    start, loop = stream_weights(list_ref, groups, w_hbm, buf, sems, compute)
    start()
    whole = pltpu.make_async_copy(t_hbm, tiles, t_sem)
    whole.start()
    planes = surf_ref.shape[0]
    for p in range(planes):
        rows[p * nbl : (p + 1) * nbl, :] = surf_ref[p].astype(F32)
    acc[...] = jnp.zeros_like(acc)
    loop()
    for r in range(ice):
        a = acc[r]
        out_ref[0, r : r + 1, :] = 0.5 * (-0.05 * a[1:2] - a[0:1])
        out_ref[1, r : r + 1, :] = a[2:3]
        out_ref[2, r : r + 1, :] = a[3:4]

    _, levels, height, across = tiles.shape
    whole.wait()
    lane = lax.broadcasted_iota(jnp.int32, (height, BS), 1)
    cols = jnp.zeros((height, BS), F32)
    for t in range(2):
        for i in range(levels):
            c = t * levels + i
            low = pltpu.roll(tiles[t, i, :, :BS], c, 1)
            high = pltpu.roll(tiles[t, i, :, across - BS :], (BS // 2 + c + 1) % BS, 1)
            cols = jnp.where(lane == c, low, jnp.where(lane == BS // 2 + c, high, cols))
            for h in range(across // BS):
                at = h * 2 * levels + c
                row0_ref[at : at + 1, :] = tiles[t, i, 0:1, h * BS : (h + 1) * BS]
                rown_ref[at : at + 1, :] = tiles[t, i, height - 1 : height, h * BS : (h + 1) * BS]
    out_ref[3] = cols


def forward(code, lst, surf, weights, tracers, ice):
    planes, nbl = surf.shape[:2]
    _, levels, height, across = tracers.shape
    assert 4 * levels == BS and height == ice
    edge = jax.ShapeDtypeStruct((2 * levels * (across // BS), BS), F32)
    return pl.pallas_call(
        forward_kernel,
        in_specs=[SM, SM, VM, ANY, ANY],
        out_specs=[VM, VM, VM],
        out_shape=[jax.ShapeDtypeStruct((4, ice, BS), F32), edge, edge],
        scratch_shapes=[
            pltpu.VMEM((planes * nbl, BS), F32),
            pltpu.VMEM((ice, 4, BS), F32),
            pltpu.VMEM(tracers.shape, F32),
            pltpu.VMEM((FWD_SLOTS, BS, BS), BF16),
            pltpu.SemaphoreType.DMA((FWD_SLOTS,)),
            pltpu.SemaphoreType.DMA(()),
        ],
        compiler_params=params(12),
        name="forward",
    )(code, lst, surf, in_hbm(weights), in_hbm(tracers))


def icerows_kernel(u_ref, wind_ref, rate_ref, strength_ref, x_ref):
    ice = rate_ref.shape[0]
    for r in range(ice):
        for c in range(2):
            x_ref[2 + c, r : r + 1, :] = u_ref[c : c + 1, r * BS : (r + 1) * BS]
            x_ref[c, r : r + 1, :] = wind_ref[c : c + 1, r * BS : (r + 1) * BS]
    rate = rate_ref[...]
    for c in range(2):
        x_ref[c] = rate * x_ref[2 + c] + x_ref[c]
    x_ref[4] = rate
    x_ref[5] = strength_ref[...]


def ice_rows(u, wind, rate, strength):
    return pl.pallas_call(
        icerows_kernel,
        in_specs=[VM] * 4,
        out_specs=VM,
        out_shape=jax.ShapeDtypeStruct((6,) + rate.shape, F32),
        compiler_params=params(2),
        name="icerows",
    )(u, wind, rate, strength)


def combine_kernel(ocn_ref, *refs):
    parts = refs[:-4]
    rows_ref, x_ref, rem_ref, cols_ref = refs[-4:]
    me, n = ocn_ref[0], len(parts)
    vals = [p[0:3] for p in parts]
    while len(vals) > 1:
        vals = [a + b for a, b in zip(vals[0::2], vals[1::2])]
    rem_ref[...] = vals[0]
    x_ref[...] = rows_ref[...]
    for c in range(2):
        x_ref[c] = rows_ref[c] + vals[0][1 + c]
    to_east = jnp.where(me < n - 1, me ^ (me + 1), 0)
    to_west = jnp.where(me > 0, me ^ (me - 1), 0)
    east = jnp.zeros(cols_ref.shape, F32)
    west = east
    for k in range(1, n):
        east = jnp.where(to_east == k, parts[k][3], east)
        west = jnp.where(to_west == k, parts[k][3], west)
    lane = lax.broadcasted_iota(jnp.int32, cols_ref.shape, 1)
    cols_ref[...] = jnp.where(lane < BS // 2, east, west)


def combine(ocn, parts, rows):
    ice = rows.shape[1]
    return pl.pallas_call(
        combine_kernel,
        in_specs=[SM] + [VM] * (len(parts) + 1),
        out_specs=[VM, VM, VM],
        out_shape=[
            jax.ShapeDtypeStruct((6, ice, BS), F32),
            jax.ShapeDtypeStruct((3, ice, BS), F32),
            jax.ShapeDtypeStruct((ice, BS), F32),
        ],
        compiler_params=params(2),
        name="combine",
    )(ocn, *parts, rows)


def solve_kernel(dst_ref, list_ref, me_ref, x_ref, rem_ref, row0_ref, rown_ref, w_hbm, *refs):
    groups_n, _, ice, _ = x_ref.shape
    outs = refs[:groups_n]
    ice_ref, fin, flux, back, buf, sems = refs[groups_n:]
    entries = dst_ref.shape[0]
    per_block = entries // ice
    nbl = outs[0].shape[0] // 3
    count = list_ref[entries + UNROLL]
    groups = lax.div(count + UNROLL - 1, UNROLL)

    def compute(base, slot):
        for q in range(UNROLL):
            e = list_ref[base + q]
            s = jnp.where(base + q < count, flux[lax.div(e, per_block)], 0.0).astype(BF16)
            part = lax.dot_general(
                s, buf[slot + q], (((1,), (0,)), ((), ())), preferred_element_type=F32
            )
            at = dst_ref[e]
            for f in range(3):
                back[f, pl.ds(at, 1), :] = back[f, pl.ds(at, 1), :] + part[f : f + 1]

    start, loop = stream_weights(list_ref, groups, w_hbm, buf, sems, compute)
    start()
    back[...] = jnp.zeros_like(back)

    n_rows = groups_n * ice
    total = 2.0 * n_rows * BS

    def plane(c):
        return jnp.concatenate([x_ref[a, c] for a in range(groups_n)], axis=0)

    base = [plane(0), plane(1)]
    current = [plane(2), plane(3)]
    rate1 = plane(4) + 1.0
    half_strength = 0.5 * plane(5)
    lane = lax.broadcasted_iota(jnp.int32, (n_rows, BS), 1)
    row = lax.broadcasted_iota(jnp.int32, (n_rows, BS), 0)

    def picard(u):
        left, right = [], []
        for z in u:
            a = pltpu.roll(z, 1, 1)
            b = pltpu.roll(a, 1, 0)
            b = jnp.where(row == 0, 0.0, b)
            left.append(jnp.where(lane == 0, b, a))
            a = pltpu.roll(z, BS - 1, 1)
            b = pltpu.roll(a, n_rows - 1, 0)
            b = jnp.where(row == n_rows - 1, 0.0, b)
            right.append(jnp.where(lane == BS - 1, b, a))
        sx = 0.5 * (right[0] - left[0])
        sy = 0.5 * (right[1] - left[1])
        zeta = half_strength / jnp.sqrt(sx * sx + sy * sy + 0.25)
        den = 1.0 / (rate1 + 2.0 * zeta)
        return [(base[c] + zeta * (left[c] + right[c])) * den for c in range(2)]

    def dot(a, b):
        return jnp.sum(a[0] * b[0] + a[1] * b[1], keepdims=True) / total

    gvals, fvals, df, dg, gram, norms = [], [], [], [], {}, []
    for step in range(ITERS):
        gnew = picard(current)
        f = [gnew[c] - current[c] for c in range(2)]
        if step == 0:
            gvals, fvals = gnew, f
            current = gnew
            continue
        df.append([f[c] - fvals[c] for c in range(2)])
        dg.append([gnew[c] - gvals[c] for c in range(2)])
        gvals, fvals = gnew, f
        j = step - 1
        for i in range(j + 1):
            gram[i, j] = dot(df[i], df[j])
        norms.append(jnp.sqrt(gram[j, j] + 1e-06))
        used = list(range(max(0, step - DEPTH), step))
        m = len(used)
        a = [[None] * m for _ in range(m)]
        for p in range(m):
            for q in range(p + 1):
                i, k = used[q], used[p]
                a[p][q] = gram[i, k] / (norms[i] * norms[k])
            a[p][p] = a[p][p] + 0.1
        h = [dot(df[i], f) / norms[i] for i in used]
        d = [None] * m
        low = [[None] * m for _ in range(m)]
        y = [None] * m
        for p in range(m):
            acc = h[p]
            for q in range(p):
                v = a[p][q]
                for s in range(q):
                    v = v - low[p][s] * low[q][s] * d[s]
                low[p][q] = v / d[q]
                acc = acc - low[p][q] * y[q]
            v = a[p][p]
            for s in range(p):
                v = v - low[p][s] * low[p][s] * d[s]
            d[p] = v
            y[p] = acc
        coef = [None] * m
        for p in reversed(range(m)):
            v = y[p] / d[p]
            for q in range(p + 1, m):
                v = v - low[q][p] * coef[q]
            coef[p] = v
        current = list(gnew)
        for p, i in enumerate(used):
            scale = coef[p] / norms[i]
            for c in range(2):
                current[c] = current[c] - scale * dg[i][c]
    fin[0] = current[0]
    fin[1] = current[1]
    mine = pl.multiple_of(me_ref[0] * ice, ice)
    own = [fin[c, pl.ds(mine, ice), :] for c in range(2)]
    planes = [own[0] - rem_ref[1], own[1] - rem_ref[2], rem_ref[0]]
    for r in range(ice):
        for c in range(2):
            ice_ref[c : c + 1, r * BS : (r + 1) * BS] = own[c][r : r + 1]
        for f in range(3):
            flux[r, f : f + 1, :] = planes[f][r : r + 1]
        flux[r, 3:4, :] = jnp.zeros((1, BS), F32)
    loop()
    for k in range(groups_n):
        for f in range(3):
            outs[k][f * nbl : (f + 1) * nbl, :] = back[f, k * nbl : (k + 1) * nbl, :]
    outs[1][3 * nbl :, :] = rown_ref[...]
    outs[groups_n - 1][3 * nbl :, :] = row0_ref[...]


def solve(dst, lst, me, x, rem, row0, rown, weights, nbl):
    groups_n, _, ice, _ = x.shape
    assert groups_n > 2
    extra = [row0.shape[0] if k in (1, groups_n - 1) else 0 for k in range(groups_n)]
    chunks = [jax.ShapeDtypeStruct((3 * nbl + e, BS), F32) for e in extra]
    return pl.pallas_call(
        solve_kernel,
        in_specs=[SM, SM, SM, VM, VM, VM, VM, ANY],
        out_specs=[VM] * (groups_n + 1),
        out_shape=chunks + [jax.ShapeDtypeStruct((2, ice * BS), F32)],
        scratch_shapes=[
            pltpu.VMEM((2, groups_n * ice, BS), F32),
            pltpu.VMEM((ice, 4, BS), F32),
            pltpu.VMEM((3, groups_n * nbl, BS), F32),
            pltpu.VMEM((BWD_SLOTS, BS, BS), BF16),
            pltpu.SemaphoreType.DMA((BWD_SLOTS,)),
        ],
        compiler_params=params(14),
        name="solve",
    )(dst, lst, me, x, rem, row0, rown, in_hbm(weights))


def finish_kernel(*refs):
    chunks = refs[:-3]
    t_ref, flux_ref, out_ref = refs[-3:]
    height, across = t_ref.shape[2:]
    for f in range(3):
        for h in range(across // BS):
            at = (f * (across // BS) + h) * height
            v = chunks[0][at : at + height, :]
            for c in chunks[1:]:
                v = v + c[at : at + height, :]
            flux_ref[f, :, h * BS : (h + 1) * BS] = v
    out_ref[0, 0] = t_ref[0, 0] + 0.5 * flux_ref[2]


def finish(chunks, tracers_next):
    height, across = tracers_next.shape[2:]
    level = pl.BlockSpec((1, 1, height, across), lambda i: (0, 0, 0, 0))
    return pl.pallas_call(
        finish_kernel,
        grid=(1,),
        in_specs=[VM] * len(chunks) + [level],
        out_specs=[pl.BlockSpec((3, height, across), lambda i: (0, 0, 0)), level],
        out_shape=[
            jax.ShapeDtypeStruct((3, height, across), F32),
            jax.ShapeDtypeStruct(tracers_next.shape, F32),
        ],
        input_output_aliases={len(chunks): 1},
        compiler_params=params(4),
        name="finish",
    )(*chunks, tracers_next)


def coupled_step(
    tracers,
    velocity,
    remap_weights,
    remap_blocks,
    remap_count,
    ice_velocity,
    ice_mass_rate,
    ice_strength,
    wind_stress,
):
    n_grp = lax.axis_size("grp")
    n_ocn = lax.axis_size("ocn")
    column = lax.axis_index("ocn")
    me = lax.axis_index("grp")
    height, across = tracers.shape[2:]
    halves = across // BS
    nbl = height * halves
    ice, per_block = remap_blocks.shape
    weights = remap_weights.reshape(ice * per_block, BS, BS)

    local = remap_blocks % (n_grp * nbl)
    tile = local // nbl
    j = local % nbl
    place = (j % halves) * height + j // halves
    mine = (jnp.arange(per_block)[None, :] < remap_count[:, None]) & (
        remap_blocks // (n_grp * nbl) == column
    )
    code = jnp.where(mine, tile * (4 * nbl) + place, -1).reshape(-1)
    dst = (((tile - me) % n_grp) * nbl + place).reshape(-1)

    surf, lst = pack_surface(code, tracers, velocity)
    surf = lax.all_gather(surf, "grp", axis=0, tiled=True)
    part, row0, rown = forward(code, lst, surf, weights, tracers, ice)
    assert n_ocn & (n_ocn - 1) == 0
    parts = [part]
    for k in range(1, n_ocn):
        parts.append(lax.ppermute(part, "ocn", [(i, i ^ k) for i in range(n_ocn)]))
    rows = ice_rows(
        ice_velocity,
        wind_stress,
        ice_mass_rate.reshape(ice, BS),
        ice_strength.reshape(ice, BS),
    )
    x, rem, cols = combine(column.reshape(1), parts, rows)
    xg = lax.all_gather(x, "grp", axis=0)
    *chunks, ice_final = solve(dst, lst, me.reshape(1), xg, rem, row0, rown, weights, nbl)
    moved = {0: chunks[0]}
    for k in [1, n_grp - 1] + list(range(2, n_grp - 1)):
        ring = [(i, (i + k) % n_grp) for i in range(n_grp)]
        moved[k] = lax.ppermute(chunks[k], "grp", ring)
    tracers_next = stencil(me.reshape(1), n_grp, tracers, velocity, moved[1], moved[n_grp - 1], cols)
    surface_flux, tracers_next = finish([moved[k] for k in range(n_grp)], tracers_next)
    return tracers_next, surface_flux, ice_final


def solution(mesh):
    return jax.shard_map(
        coupled_step,
        mesh=mesh,
        in_specs=(
            P(None, None, "grp", "ocn"),
            P(None, None, "grp", "ocn"),
            P("grp", None, None, None),
            P("grp", None),
            P("grp"),
            P(None, "grp"),
            P("grp"),
            P("grp"),
            P(None, "grp"),
        ),
        out_specs=(P(None, None, "grp", "ocn"), P(None, "grp", "ocn"), P(None, "grp")),
        check_vma=False,
    )
```

```python
import functools

import jax
import jax.numpy as jnp
from jax import lax
from jax.experimental import pallas as pl
from jax.experimental.pallas import tpu as pltpu
from jax.sharding import PartitionSpec as P


BS = 128
ITERS = 4
DEPTH = 3
UNROLL = 8
FWD_SLOTS = 32
BWD_SLOTS = 64
F32 = jnp.float32
BF16 = jnp.bfloat16


VM = pl.BlockSpec(memory_space=pltpu.VMEM)
SM = pl.BlockSpec(memory_space=pltpu.SMEM)
ANY = pl.BlockSpec(memory_space=pltpu.HBM)


def in_hbm(x):
    return pltpu.with_memory_space_constraint(x, pltpu.HBM)


def params(mib):
    return pltpu.CompilerParams(vmem_limit_bytes=mib * 1024 * 1024)


def surface_kernel(code_ref, t_hbm, v_hbm, out_ref, list_ref, buf, sems):
    height, across = buf.shape[1:]
    entries = code_ref.shape[0]
    copies = [
        pltpu.make_async_copy(
            (t_hbm if f < 2 else v_hbm).at[f % 2, 0], buf.at[f], sems.at[f]
        )
        for f in range(4)
    ]
    for c in copies:
        c.start()

    def scan(i, n):
        for q in range(8):
            e = i * 8 + q
            list_ref[n] = e
            n = n + jnp.where(code_ref[e] >= 0, 1, 0)
        return n

    count = lax.fori_loop(0, entries // 8, scan, 0)
    for q in range(UNROLL):
        list_ref[count + q] = 0
    list_ref[entries + UNROLL] = count
    for c in copies:
        c.wait()
    for f in range(4):
        for h in range(across // BS):
            out_ref[f, h * height : (h + 1) * height, :] = buf[
                f, :, h * BS : (h + 1) * BS
            ].astype(BF16)


def pack_surface(code, tracers, velocity):
    height, across = tracers.shape[2:]
    nbl = height * across // BS
    return pl.pallas_call(
        surface_kernel,
        in_specs=[SM, ANY, ANY],
        out_specs=[VM, SM],
        out_shape=[
            jax.ShapeDtypeStruct((4, nbl, BS), BF16),
            jax.ShapeDtypeStruct((code.shape[0] + UNROLL + 8,), jnp.int32),
        ],
        scratch_shapes=[
            pltpu.VMEM((4, height, across), F32),
            pltpu.SemaphoreType.DMA((4,)),
        ],
        compiler_params=params(4),
        name="surface",
    )(code, in_hbm(tracers), in_hbm(velocity))


def stencil_kernel(
    n_grp, me_ref, t_ref, up_ref, dn_ref, v_ref, south_ref, north_ref, cols_ref, out_ref, level_ref
):
    step = pl.program_id(0)
    steps = pl.num_programs(0)
    lc, height, across = t_ref.shape[1:]
    halves = across // BS
    levels = lc * steps
    skip = south_ref.shape[0] - 2 * levels * halves
    lane = lax.broadcasted_iota(jnp.int32, (height, across), 1)
    row = lax.broadcasted_iota(jnp.int32, (height, across), 0)
    pad = jnp.zeros((height, across - BS), F32)
    top = jnp.where(step == 0, 0.0, 1.0)
    bottom = jnp.where(step == steps - 1, 0.0, 1.0)
    no_south = jnp.where(me_ref[0] == 0, 0.0, 1.0)
    no_north = jnp.where(me_ref[0] == n_grp - 1, 0.0, 1.0)

    def outer_row(ref, c):
        pieces = [ref[pl.ds(skip + h * 2 * levels + c, 1), :] for h in range(halves)]
        return jnp.concatenate(pieces, axis=1)

    for i in range(lc):
        u = v_ref[0, i]
        v = v_ref[1, i]
        for t in range(2):
            c = t * levels + step * lc + i
            x = t_ref[t, i]
            above = up_ref[t, 0] * top if i == 0 else t_ref[t, i - 1]
            below = dn_ref[t, 0] * bottom if i == lc - 1 else t_ref[t, i + 1]
            cols = cols_ref[...]
            wcol = jnp.concatenate([pltpu.roll(cols, BS // 2 - c, 1), pad], axis=1)
            ecol = jnp.concatenate([pad, pltpu.roll(cols, BS - 1 - c, 1)], axis=1)
            south = outer_row(south_ref, c) * no_south
            north = outer_row(north_ref, c) * no_north
            w = jnp.where(lane == 0, wcol, pltpu.roll(x, 1, 1))
            e = jnp.where(lane == across - 1, ecol, pltpu.roll(x, across - 1, 1))
            s = jnp.where(row == 0, south, pltpu.roll(x, 1, 0))
            n = jnp.where(row == height - 1, north, pltpu.roll(x, height - 1, 0))
            advect = u * (e - w) * 0.5 + v * (n - s) * 0.5
            new = (
                x
                + 0.2 * (e + w + n + s - 4.0 * x)
                - 0.5 * advect
                + 0.2 * (above + below - 2.0 * x)
            )
            out_ref[t, i] = new
            if t == 0 and i == 0:

                @pl.when(step == 0)
                def _():
                    level_ref[...] = new


def stencil(me, n_grp, tracers, velocity, south, north, cols):
    _, levels, height, across = tracers.shape
    lc = 8
    main = pl.BlockSpec((2, lc, height, across), lambda i: (0, i, 0, 0))
    up = pl.BlockSpec((2, 1, height, across), lambda i: (0, jnp.maximum(i * lc - 1, 0), 0, 0))
    dn = pl.BlockSpec(
        (2, 1, height, across), lambda i: (0, jnp.minimum(i * lc + lc, levels - 1), 0, 0)
    )
    return pl.pallas_call(
        functools.partial(stencil_kernel, n_grp),
        grid=(levels // lc,),
        in_specs=[SM, main, up, dn, main, VM, VM, VM],
        out_specs=[main, pl.BlockSpec((height, across), lambda i: (0, 0))],
        out_shape=[
            jax.ShapeDtypeStruct(tracers.shape, F32),
            jax.ShapeDtypeStruct((height, across), F32),
        ],
        compiler_params=params(14),
        cost_estimate=pl.CostEstimate(
            flops=120_000_000, bytes_accessed=4 * tracers.size * 4, transcendentals=0
        ),
        name="stencil",
    )(me, tracers, tracers, tracers, velocity, south, north, cols)


def stream_weights(list_ref, groups, w_hbm, buf, sems, compute):
    slots = buf.shape[0]

    def copy(i, slot):
        return pltpu.make_async_copy(w_hbm.at[list_ref[i]], buf.at[slot], sems.at[slot])

    def start():
        for s in range(slots // UNROLL):

            @pl.when(s < groups)
            def _():
                for q in range(UNROLL):
                    copy(s * UNROLL + q, s * UNROLL + q).start()

    def loop():
        def body(g, carry):
            base = g * UNROLL
            slot = lax.rem(g, slots // UNROLL) * UNROLL
            for q in range(UNROLL):
                copy(base + q, slot + q).wait()
            compute(base, slot)

            @pl.when(g + slots // UNROLL < groups)
            def _():
                for q in range(UNROLL):
                    copy(base + slots + q, slot + q).start()

            return carry

        lax.fori_loop(0, groups, body, 0)

    return start, loop


def edge_partners(n):
    return [k for k in range(1, n) if k & (k + 1) == 0]


def forward_kernel(n_ocn, code_ref, list_ref, ocn_ref, surf_ref, w_hbm, tiles, *refs):
    ks = edge_partners(n_ocn)
    out_ref, row0_ref, rown_ref = refs[:3]
    sends = refs[3 : 3 + len(ks)]
    rows, acc, buf, sems = refs[3 + len(ks) :]
    entries = code_ref.shape[0]
    ice = acc.shape[0]
    per_block = entries // ice
    nbl = surf_ref.shape[1]
    count = list_ref[entries + UNROLL]
    groups = lax.div(count + UNROLL - 1, UNROLL)
    first = lax.broadcasted_iota(jnp.int32, (4, BS), 0)

    def compute(base, slot):
        for q in range(UNROLL):
            e = list_ref[base + q]
            at = jnp.maximum(code_ref[e], 0)
            r0 = jnp.broadcast_to(rows[pl.ds(at, 1), :], (4, BS))
            r1 = jnp.broadcast_to(rows[pl.ds(at + nbl, 1), :], (4, BS))
            r2 = jnp.broadcast_to(rows[pl.ds(at + 2 * nbl, 1), :], (4, BS))
            r3 = jnp.broadcast_to(rows[pl.ds(at + 3 * nbl, 1), :], (4, BS))
            s = jnp.where(first == 0, r0, jnp.where(first == 1, r1, jnp.where(first == 2, r2, r3)))
            s = jnp.where(base + q < count, s, 0.0).astype(BF16)
            part = lax.dot_general(
                s, buf[slot + q], (((1,), (1,)), ((), ())), preferred_element_type=F32
            )
            r = lax.div(e, per_block)
            acc[r] = acc[r] + part

    start, loop = stream_weights(list_ref, groups, w_hbm, buf, sems, compute)
    start()
    planes = surf_ref.shape[0]
    for p in range(planes):
        rows[p * nbl : (p + 1) * nbl, :] = surf_ref[p].astype(F32)
    acc[...] = jnp.zeros_like(acc)
    loop()
    for r in range(ice):
        a = acc[r]
        out_ref[r : r + 1, :] = 0.5 * (-0.05 * a[1:2] - a[0:1])
        out_ref[ice + r : ice + r + 1, :] = a[2:3]
        out_ref[2 * ice + r : 2 * ice + r + 1, :] = a[3:4]

    _, levels, height, across = tiles.shape
    lane = lax.broadcasted_iota(jnp.int32, (height, BS), 1)
    cols = jnp.zeros((height, BS), F32)
    for t in range(2):
        for i in range(levels):
            c = t * levels + i
            low = pltpu.roll(tiles[t, i, :, :BS], c, 1)
            high = pltpu.roll(tiles[t, i, :, across - BS :], (BS // 2 + c + 1) % BS, 1)
            cols = jnp.where(lane == c, low, jnp.where(lane == BS // 2 + c, high, cols))
            for h in range(across // BS):
                at = h * 2 * levels + c
                row0_ref[at : at + 1, :] = tiles[t, i, 0:1, h * BS : (h + 1) * BS]
                rown_ref[at : at + 1, :] = tiles[t, i, height - 1 : height, h * BS : (h + 1) * BS]
    half = height // 2
    side = lane[:half] < BS // 2
    turned = pltpu.roll(cols, BS // 2, 1)
    low = jnp.where(side, cols[:half], turned[half:])
    high = jnp.where(side, turned[:half], cols[half:])
    me = ocn_ref[0]
    for k, send in zip(ks, sends):
        send[0 : 3 * ice, :] = out_ref[...]
        send[3 * ice :, :] = jnp.where((me ^ k) == me + 1, high, low)


def forward(code, lst, ocn, n_ocn, surf, weights, tracers, ice):
    planes, nbl = surf.shape[:2]
    _, levels, height, across = tracers.shape
    assert 4 * levels == BS and height == ice
    edge = jax.ShapeDtypeStruct((2 * levels * (across // BS), BS), F32)
    ks = edge_partners(n_ocn)
    send = jax.ShapeDtypeStruct((3 * ice + height // 2, BS), F32)
    return pl.pallas_call(
        functools.partial(forward_kernel, n_ocn),
        in_specs=[SM, SM, SM, VM, ANY, VM],
        out_specs=[VM] * (3 + len(ks)),
        out_shape=[jax.ShapeDtypeStruct((3 * ice, BS), F32), edge, edge] + [send] * len(ks),
        scratch_shapes=[
            pltpu.VMEM((planes * nbl, BS), F32),
            pltpu.VMEM((ice, 4, BS), F32),
            pltpu.VMEM((FWD_SLOTS, BS, BS), BF16),
            pltpu.SemaphoreType.DMA((FWD_SLOTS,)),
        ],
        compiler_params=params(12),
        name="forward",
    )(code, lst, ocn, surf, in_hbm(weights), tracers)


def icerows_kernel(u_ref, wind_ref, rate_ref, strength_ref, x_ref):
    ice = rate_ref.shape[0]
    for r in range(ice):
        for c in range(2):
            x_ref[2 + c, r : r + 1, :] = u_ref[c : c + 1, r * BS : (r + 1) * BS]
            x_ref[c, r : r + 1, :] = wind_ref[c : c + 1, r * BS : (r + 1) * BS]
    rate = rate_ref[...]
    for c in range(2):
        x_ref[c] = rate * x_ref[2 + c] + x_ref[c]
    x_ref[4] = rate
    x_ref[5] = strength_ref[...]


def ice_rows(u, wind, rate, strength):
    return pl.pallas_call(
        icerows_kernel,
        in_specs=[VM] * 4,
        out_specs=VM,
        out_shape=jax.ShapeDtypeStruct((6,) + rate.shape, F32),
        compiler_params=params(2),
        name="icerows",
    )(u, wind, rate, strength)


def combine_kernel(ocn_ref, *refs):
    parts = refs[:-4]
    rows_ref, x_ref, rem_ref, cols_ref = refs[-4:]
    me, n = ocn_ref[0], len(parts)
    ice = rem_ref.shape[1]
    vals = [[p[c * ice : (c + 1) * ice, :] for c in range(3)] for p in parts]
    while len(vals) > 1:
        vals = [[x + y for x, y in zip(a, b)] for a, b in zip(vals[0::2], vals[1::2])]
    x_ref[...] = rows_ref[...]
    for c in range(3):
        rem_ref[c] = vals[0][c]
    for c in range(2):
        x_ref[c] = rows_ref[c] + vals[0][1 + c]
    to_east = jnp.where(me < n - 1, me ^ (me + 1), 0)
    to_west = jnp.where(me > 0, me ^ (me - 1), 0)
    east = jnp.zeros((cols_ref.shape[0] // 2, BS), F32)
    west = east
    for k in edge_partners(n):
        east = jnp.where(to_east == k, parts[k][3 * ice :, :], east)
        west = jnp.where(to_west == k, parts[k][3 * ice :, :], west)
    east = jnp.concatenate([east, pltpu.roll(east, BS // 2, 1)], axis=0)
    west = jnp.concatenate([pltpu.roll(west, BS // 2, 1), west], axis=0)
    lane = lax.broadcasted_iota(jnp.int32, cols_ref.shape, 1)
    cols_ref[...] = jnp.where(lane < BS // 2, east, west)


def combine(ocn, parts, rows):
    ice = rows.shape[1]
    return pl.pallas_call(
        combine_kernel,
        in_specs=[SM] + [VM] * (len(parts) + 1),
        out_specs=[VM, VM, VM],
        out_shape=[
            jax.ShapeDtypeStruct((6, ice, BS), F32),
            jax.ShapeDtypeStruct((3, ice, BS), F32),
            jax.ShapeDtypeStruct((ice, BS), F32),
        ],
        compiler_params=params(2),
        name="combine",
    )(ocn, *parts, rows)


def solve_kernel(dst_ref, list_ref, me_ref, x_ref, rem_ref, row0_ref, rown_ref, w_hbm, *refs):
    groups_n, _, ice, _ = x_ref.shape
    outs = refs[:groups_n]
    ice_ref, fin, flux, back, buf, sems = refs[groups_n:]
    entries = dst_ref.shape[0]
    per_block = entries // ice
    nbl = outs[0].shape[0] // 3
    count = list_ref[entries + UNROLL]
    groups = lax.div(count + UNROLL - 1, UNROLL)

    def compute(base, slot):
        for q in range(UNROLL):
            e = list_ref[base + q]
            s = jnp.where(base + q < count, flux[lax.div(e, per_block)], 0.0).astype(BF16)
            part = lax.dot_general(
                s, buf[slot + q], (((1,), (0,)), ((), ())), preferred_element_type=F32
            )
            at = dst_ref[e]
            for f in range(3):
                back[f, pl.ds(at, 1), :] = back[f, pl.ds(at, 1), :] + part[f : f + 1]

    start, loop = stream_weights(list_ref, groups, w_hbm, buf, sems, compute)
    start()
    back[...] = jnp.zeros_like(back)

    n_rows = groups_n * ice
    total = 2.0 * n_rows * BS

    def plane(c):
        return jnp.concatenate([x_ref[a, c] for a in range(groups_n)], axis=0)

    base = [plane(0), plane(1)]
    current = [plane(2), plane(3)]
    rate1 = plane(4) + 1.0
    strength = plane(5)
    strength2 = 2.0 * strength
    lane = lax.broadcasted_iota(jnp.int32, (n_rows, BS), 1)
    corner = lax.broadcasted_iota(jnp.int32, (8, BS), 0) * BS + lane[:8]

    def picard(u):
        left, right = [], []
        for z in u:
            a = pltpu.roll(z, 1, 1)
            a = jnp.where(lane == 0, pltpu.roll(a, 1, 0), a)
            left.append(jnp.concatenate([jnp.where(corner == 0, 0.0, a[:8]), a[8:]], axis=0))
            a = pltpu.roll(z, BS - 1, 1)
            a = jnp.where(lane == BS - 1, pltpu.roll(a, n_rows - 1, 0), a)
            end = jnp.where(corner == 8 * BS - 1, 0.0, a[n_rows - 8 :])
            right.append(jnp.concatenate([a[: n_rows - 8], end], axis=0))
        dx = right[0] - left[0]
        dy = right[1] - left[1]
        d = dx * dx + dy * dy + 1.0
        q = d * lax.rsqrt(d)
        inverse = 1.0 / (rate1 * q + strength2)
        return [(base[c] * q + strength * (left[c] + right[c])) * inverse for c in range(2)]

    def dot(a, b):
        return jnp.sum(a[0] * b[0] + a[1] * b[1], keepdims=True) / total

    gvals, fvals, df, dg, gram, norms = [], [], [], [], {}, []
    for step in range(ITERS):
        gnew = picard(current)
        f = [gnew[c] - current[c] for c in range(2)]
        if step == 0:
            gvals, fvals = gnew, f
            current = gnew
            continue
        df.append([f[c] - fvals[c] for c in range(2)])
        dg.append([gnew[c] - gvals[c] for c in range(2)])
        gvals, fvals = gnew, f
        j = step - 1
        for i in range(j + 1):
            gram[i, j] = dot(df[i], df[j])
        norms.append(jnp.sqrt(gram[j, j] + 1e-06))
        used = list(range(max(0, step - DEPTH), step))
        m = len(used)
        a = [[None] * m for _ in range(m)]
        for p in range(m):
            for q in range(p + 1):
                i, k = used[q], used[p]
                a[p][q] = gram[i, k] / (norms[i] * norms[k])
            a[p][p] = a[p][p] + 0.1
        h = [dot(df[i], f) / norms[i] for i in used]
        d = [None] * m
        low = [[None] * m for _ in range(m)]
        y = [None] * m
        for p in range(m):
            acc = h[p]
            for q in range(p):
                v = a[p][q]
                for s in range(q):
                    v = v - low[p][s] * low[q][s] * d[s]
                low[p][q] = v / d[q]
                acc = acc - low[p][q] * y[q]
            v = a[p][p]
            for s in range(p):
                v = v - low[p][s] * low[p][s] * d[s]
            d[p] = v
            y[p] = acc
        coef = [None] * m
        for p in reversed(range(m)):
            v = y[p] / d[p]
            for q in range(p + 1, m):
                v = v - low[q][p] * coef[q]
            coef[p] = v
        current = list(gnew)
        for p, i in enumerate(used):
            scale = coef[p] / norms[i]
            for c in range(2):
                current[c] = current[c] - scale * dg[i][c]
    fin[0] = current[0]
    fin[1] = current[1]
    mine = pl.multiple_of(me_ref[0] * ice, ice)
    own = [fin[c, pl.ds(mine, ice), :] for c in range(2)]
    planes = [own[0] - rem_ref[1], own[1] - rem_ref[2], rem_ref[0]]
    for r in range(ice):
        for c in range(2):
            ice_ref[c : c + 1, r * BS : (r + 1) * BS] = own[c][r : r + 1]
        for f in range(3):
            flux[r, f : f + 1, :] = planes[f][r : r + 1]
        flux[r, 3:4, :] = jnp.zeros((1, BS), F32)
    loop()
    for k in range(groups_n):
        for f in range(3):
            outs[k][f * nbl : (f + 1) * nbl, :] = back[f, k * nbl : (k + 1) * nbl, :]
    outs[1][3 * nbl :, :] = rown_ref[...]
    outs[groups_n - 1][3 * nbl :, :] = row0_ref[...]


def solve(dst, lst, me, x, rem, row0, rown, weights, nbl):
    groups_n, _, ice, _ = x.shape
    assert groups_n > 2
    extra = [row0.shape[0] if k in (1, groups_n - 1) else 0 for k in range(groups_n)]
    chunks = [jax.ShapeDtypeStruct((3 * nbl + e, BS), F32) for e in extra]
    return pl.pallas_call(
        solve_kernel,
        in_specs=[SM, SM, SM, VM, VM, VM, VM, ANY],
        out_specs=[VM] * (groups_n + 1),
        out_shape=chunks + [jax.ShapeDtypeStruct((2, ice * BS), F32)],
        scratch_shapes=[
            pltpu.VMEM((2, groups_n * ice, BS), F32),
            pltpu.VMEM((ice, 4, BS), F32),
            pltpu.VMEM((3, groups_n * nbl, BS), F32),
            pltpu.VMEM((BWD_SLOTS, BS, BS), BF16),
            pltpu.SemaphoreType.DMA((BWD_SLOTS,)),
        ],
        compiler_params=params(14),
        name="solve",
    )(dst, lst, me, x, rem, row0, rown, in_hbm(weights))


def finish_kernel(*refs):
    chunks = refs[:-6]
    level_ref, _, flux_ref, out_hbm, buf, sem = refs[-6:]
    height, across = level_ref.shape
    put = pltpu.make_async_copy(buf, out_hbm.at[0, 0], sem)
    for f in (2, 0, 1):
        for h in range(across // BS):
            at = (f * (across // BS) + h) * height
            v = chunks[0][at : at + height, :]
            for c in chunks[1:]:
                v = v + c[at : at + height, :]
            flux_ref[f, :, h * BS : (h + 1) * BS] = v
            if f == 2:
                cols = slice(h * BS, (h + 1) * BS)
                buf[:, cols] = level_ref[:, cols] + 0.5 * v
        if f == 2:
            put.start()
    put.wait()


def finish(chunks, level, tracers_next):
    height, across = level.shape
    return pl.pallas_call(
        finish_kernel,
        in_specs=[VM] * (len(chunks) + 1) + [ANY],
        out_specs=[VM, ANY],
        out_shape=[
            jax.ShapeDtypeStruct((3, height, across), F32),
            jax.ShapeDtypeStruct(tracers_next.shape, F32),
        ],
        scratch_shapes=[pltpu.VMEM((height, across), F32), pltpu.SemaphoreType.DMA(())],
        input_output_aliases={len(chunks) + 1: 1},
        compiler_params=params(4),
        name="finish",
    )(*chunks, level, in_hbm(tracers_next))


def coupled_step(
    tracers,
    velocity,
    remap_weights,
    remap_blocks,
    remap_count,
    ice_velocity,
    ice_mass_rate,
    ice_strength,
    wind_stress,
):
    n_grp = lax.axis_size("grp")
    n_ocn = lax.axis_size("ocn")
    column = lax.axis_index("ocn")
    me = lax.axis_index("grp")
    height, across = tracers.shape[2:]
    halves = across // BS
    nbl = height * halves
    ice, per_block = remap_blocks.shape
    weights = remap_weights.reshape(ice * per_block, BS, BS)

    local = remap_blocks % (n_grp * nbl)
    tile = local // nbl
    j = local % nbl
    place = (j % halves) * height + j // halves
    mine = (jnp.arange(per_block)[None, :] < remap_count[:, None]) & (
        remap_blocks // (n_grp * nbl) == column
    )
    code = jnp.where(mine, tile * (4 * nbl) + place, -1).reshape(-1)
    dst = (((tile - me) % n_grp) * nbl + place).reshape(-1)

    surf, lst = pack_surface(code, tracers, velocity)
    surf = lax.all_gather(surf, "grp", axis=0, tiled=True)
    assert n_ocn & (n_ocn - 1) == 0
    ocn = column.reshape(1)
    part, row0, rown, *sends = forward(code, lst, ocn, n_ocn, surf, weights, tracers, ice)
    sends = dict(zip(edge_partners(n_ocn), sends))
    parts = [part]
    for k in range(1, n_ocn):
        pairs = [(i, i ^ k) for i in range(n_ocn)]
        parts.append(lax.ppermute(sends.get(k, part), "ocn", pairs))
    rows = ice_rows(
        ice_velocity,
        wind_stress,
        ice_mass_rate.reshape(ice, BS),
        ice_strength.reshape(ice, BS),
    )
    x, rem, cols = combine(ocn, parts, rows)
    xg = lax.all_gather(x, "grp", axis=0)
    *chunks, ice_final = solve(dst, lst, me.reshape(1), xg, rem, row0, rown, weights, nbl)
    moved = {0: chunks[0]}
    for k in [1, n_grp - 1] + list(range(2, n_grp - 1)):
        ring = [(i, (i + k) % n_grp) for i in range(n_grp)]
        moved[k] = lax.ppermute(chunks[k], "grp", ring)
    tracers_next, level = stencil(me.reshape(1), n_grp, tracers, velocity, moved[1], moved[n_grp - 1], cols)
    surface_flux, tracers_next = finish([moved[k] for k in range(n_grp)], level, tracers_next)
    return tracers_next, surface_flux, ice_final


def solution(mesh):
    return jax.shard_map(
        coupled_step,
        mesh=mesh,
        in_specs=(
            P(None, None, "grp", "ocn"),
            P(None, None, "grp", "ocn"),
            P("grp", None, None, None),
            P("grp", None),
            P("grp"),
            P(None, "grp"),
            P("grp"),
            P("grp"),
            P(None, "grp"),
        ),
        out_specs=(P(None, None, "grp", "ocn"), P(None, "grp", "ocn"), P(None, "grp")),
        check_vma=False,
    )
```

```python
import functools

import jax
import jax.numpy as jnp
from jax import lax
from jax.experimental import pallas as pl
from jax.experimental.pallas import tpu as pltpu
from jax.sharding import PartitionSpec as P


BS = 128
ITERS = 4
DEPTH = 3
UNROLL = 8
FWD_SLOTS = 32
BWD_SLOTS = 64
F32 = jnp.float32
BF16 = jnp.bfloat16


VM = pl.BlockSpec(memory_space=pltpu.VMEM)
SM = pl.BlockSpec(memory_space=pltpu.SMEM)
ANY = pl.BlockSpec(memory_space=pltpu.HBM)


def in_hbm(x):
    return pltpu.with_memory_space_constraint(x, pltpu.HBM)


def params(mib):
    return pltpu.CompilerParams(vmem_limit_bytes=mib * 1024 * 1024)


def split(v, d):
    if d & (d - 1) == 0:
        return lax.shift_right_logical(v, d.bit_length() - 1), v & (d - 1)
    return lax.div(v, d), lax.rem(v, d)


def place_of(local, height, halves):
    tile, j = split(local, height * halves)
    row, half = split(j, halves)
    return tile, half * height + row


def surface_kernel(
    n_grp, blocks_ref, count_ref, ocn_ref, t_hbm, v_hbm, out_ref, list_ref, buf, sems
):
    height, across = buf.shape[1:]
    per_block, ice = blocks_ref.shape
    room = ice * per_block + UNROLL
    size = n_grp * height * across // BS
    lowest = ocn_ref[0] * size
    copies = [
        pltpu.make_async_copy(
            (t_hbm if f < 2 else v_hbm).at[f % 2, 0], buf.at[f], sems.at[f]
        )
        for f in range(4)
    ]
    for c in copies:
        c.start()

    def scan(r, n):
        live = count_ref[r]
        for k in range(per_block):
            local = blocks_ref[k, r] - lowest
            list_ref[n] = r * per_block + k
            list_ref[room + n] = local
            n = n + jnp.where((local >= 0) & (local < size) & (k < live), 1, 0)
        return n

    count = lax.fori_loop(0, ice, scan, 0)
    for q in range(UNROLL):
        list_ref[count + q] = 0
        list_ref[room + count + q] = 0
    list_ref[2 * room] = count
    for c in copies:
        c.wait()
    for f in range(4):
        for h in range(across // BS):
            out_ref[f, h * height : (h + 1) * height, :] = buf[
                f, :, h * BS : (h + 1) * BS
            ].astype(BF16)


def pack_surface(n_grp, blocks, count, ocn, tracers, velocity):
    height, across = tracers.shape[2:]
    nbl = height * across // BS
    return pl.pallas_call(
        functools.partial(surface_kernel, n_grp),
        in_specs=[SM, SM, SM, ANY, ANY],
        out_specs=[VM, SM],
        out_shape=[
            jax.ShapeDtypeStruct((4, nbl, BS), BF16),
            jax.ShapeDtypeStruct((2 * (blocks.size + UNROLL) + 8,), jnp.int32),
        ],
        scratch_shapes=[
            pltpu.VMEM((4, height, across), F32),
            pltpu.SemaphoreType.DMA((4,)),
        ],
        compiler_params=params(4),
        name="surface",
    )(in_hbm(blocks), in_hbm(count), ocn, in_hbm(tracers), in_hbm(velocity))


def stencil_kernel(
    n_grp, me_ref, t_ref, up_ref, dn_ref, v_ref, south_ref, north_ref, cols_ref, out_ref, level_ref
):
    step = pl.program_id(0)
    steps = pl.num_programs(0)
    lc, height, across = t_ref.shape[1:]
    halves = across // BS
    levels = lc * steps
    skip = south_ref.shape[0] - 2 * levels * halves
    lane = lax.broadcasted_iota(jnp.int32, (height, across), 1)
    row = lax.broadcasted_iota(jnp.int32, (height, across), 0)
    pad = jnp.zeros((height, across - BS), F32)
    top = jnp.where(step == 0, 0.0, 1.0)
    bottom = jnp.where(step == steps - 1, 0.0, 1.0)
    no_south = jnp.where(me_ref[0] == 0, 0.0, 1.0)
    no_north = jnp.where(me_ref[0] == n_grp - 1, 0.0, 1.0)

    def outer_row(ref, c):
        pieces = [ref[pl.ds(skip + h * 2 * levels + c, 1), :] for h in range(halves)]
        return jnp.concatenate(pieces, axis=1)

    for i in range(lc):
        u = v_ref[0, i]
        v = v_ref[1, i]
        for t in range(2):
            c = t * levels + step * lc + i
            x = t_ref[t, i]
            above = up_ref[t, 0] * top if i == 0 else t_ref[t, i - 1]
            below = dn_ref[t, 0] * bottom if i == lc - 1 else t_ref[t, i + 1]
            cols = cols_ref[...]
            wcol = jnp.concatenate([pltpu.roll(cols, BS // 2 - c, 1), pad], axis=1)
            ecol = jnp.concatenate([pad, pltpu.roll(cols, BS - 1 - c, 1)], axis=1)
            south = outer_row(south_ref, c) * no_south
            north = outer_row(north_ref, c) * no_north
            w = jnp.where(lane == 0, wcol, pltpu.roll(x, 1, 1))
            e = jnp.where(lane == across - 1, ecol, pltpu.roll(x, across - 1, 1))
            s = jnp.where(row == 0, south, pltpu.roll(x, 1, 0))
            n = jnp.where(row == height - 1, north, pltpu.roll(x, height - 1, 0))
            advect = u * (e - w) * 0.5 + v * (n - s) * 0.5
            new = (
                x
                + 0.2 * (e + w + n + s - 4.0 * x)
                - 0.5 * advect
                + 0.2 * (above + below - 2.0 * x)
            )
            out_ref[t, i] = new
            if t == 0 and i == 0:

                @pl.when(step == 0)
                def _():
                    level_ref[...] = new


def stencil(me, n_grp, tracers, velocity, south, north, cols):
    _, levels, height, across = tracers.shape
    lc = 8
    main = pl.BlockSpec((2, lc, height, across), lambda i: (0, i, 0, 0))
    up = pl.BlockSpec((2, 1, height, across), lambda i: (0, jnp.maximum(i * lc - 1, 0), 0, 0))
    dn = pl.BlockSpec(
        (2, 1, height, across), lambda i: (0, jnp.minimum(i * lc + lc, levels - 1), 0, 0)
    )
    return pl.pallas_call(
        functools.partial(stencil_kernel, n_grp),
        grid=(levels // lc,),
        in_specs=[SM, main, up, dn, main, VM, VM, VM],
        out_specs=[main, pl.BlockSpec((height, across), lambda i: (0, 0))],
        out_shape=[
            jax.ShapeDtypeStruct(tracers.shape, F32),
            jax.ShapeDtypeStruct((height, across), F32),
        ],
        compiler_params=params(14),
        cost_estimate=pl.CostEstimate(
            flops=120_000_000, bytes_accessed=4 * tracers.size * 4, transcendentals=0
        ),
        name="stencil",
    )(me, tracers, tracers, tracers, velocity, south, north, cols)


def stream_weights(list_ref, groups, w_hbm, buf, sems, compute):
    slots = buf.shape[0]

    def copy(i, slot):
        return pltpu.make_async_copy(w_hbm.at[list_ref[i]], buf.at[slot], sems.at[slot])

    def start():
        for s in range(slots // UNROLL):

            @pl.when(s < groups)
            def _():
                for q in range(UNROLL):
                    copy(s * UNROLL + q, s * UNROLL + q).start()

    def loop():
        def body(g, carry):
            base = g * UNROLL
            slot = lax.rem(g, slots // UNROLL) * UNROLL
            for q in range(UNROLL):
                copy(base + q, slot + q).wait()
            compute(base, slot)

            @pl.when(g + slots // UNROLL < groups)
            def _():
                for q in range(UNROLL):
                    copy(base + slots + q, slot + q).start()

            return carry

        lax.fori_loop(0, groups, body, 0)

    return start, loop


def edge_partners(n):
    return [k for k in range(1, n) if k & (k + 1) == 0]


def forward_kernel(n_ocn, list_ref, ocn_ref, surf_ref, w_hbm, tiles, *refs):
    ks = edge_partners(n_ocn)
    out_ref, row0_ref, rown_ref = refs[:3]
    sends = refs[3 : 3 + len(ks)]
    rows, acc, buf, sems = refs[3 + len(ks) :]
    entries = w_hbm.shape[0]
    room = entries + UNROLL
    ice = acc.shape[0]
    per_block = entries // ice
    nbl = surf_ref.shape[1]
    halves = nbl // tiles.shape[2]
    count = list_ref[2 * room]
    groups = lax.div(count + UNROLL - 1, UNROLL)
    first = lax.broadcasted_iota(jnp.int32, (4, BS), 0)

    def compute(base, slot):
        for q in range(UNROLL):
            e = list_ref[base + q]
            tile, place = place_of(list_ref[room + base + q], nbl // halves, halves)
            at = tile * (4 * nbl) + place
            r0 = jnp.broadcast_to(rows[pl.ds(at, 1), :], (4, BS))
            r1 = jnp.broadcast_to(rows[pl.ds(at + nbl, 1), :], (4, BS))
            r2 = jnp.broadcast_to(rows[pl.ds(at + 2 * nbl, 1), :], (4, BS))
            r3 = jnp.broadcast_to(rows[pl.ds(at + 3 * nbl, 1), :], (4, BS))
            s = jnp.where(first == 0, r0, jnp.where(first == 1, r1, jnp.where(first == 2, r2, r3)))
            s = jnp.where(base + q < count, s, 0.0).astype(BF16)
            part = lax.dot_general(
                s, buf[slot + q], (((1,), (1,)), ((), ())), preferred_element_type=F32
            )
            r = lax.div(e, per_block)
            acc[r] = acc[r] + part

    start, loop = stream_weights(list_ref, groups, w_hbm, buf, sems, compute)
    start()
    planes = surf_ref.shape[0]
    for p in range(planes):
        rows[p * nbl : (p + 1) * nbl, :] = surf_ref[p].astype(F32)
    acc[...] = jnp.zeros_like(acc)
    loop()
    for r in range(ice):
        a = acc[r]
        out_ref[r : r + 1, :] = 0.5 * (-0.05 * a[1:2] - a[0:1])
        out_ref[ice + r : ice + r + 1, :] = a[2:3]
        out_ref[2 * ice + r : 2 * ice + r + 1, :] = a[3:4]

    _, levels, height, across = tiles.shape
    lane = lax.broadcasted_iota(jnp.int32, (height, BS), 1)
    cols = jnp.zeros((height, BS), F32)
    for t in range(2):
        for i in range(levels):
            c = t * levels + i
            low = pltpu.roll(tiles[t, i, :, :BS], c, 1)
            high = pltpu.roll(tiles[t, i, :, across - BS :], (BS // 2 + c + 1) % BS, 1)
            cols = jnp.where(lane == c, low, jnp.where(lane == BS // 2 + c, high, cols))
            for h in range(across // BS):
                at = h * 2 * levels + c
                row0_ref[at : at + 1, :] = tiles[t, i, 0:1, h * BS : (h + 1) * BS]
                rown_ref[at : at + 1, :] = tiles[t, i, height - 1 : height, h * BS : (h + 1) * BS]
    half = height // 2
    side = lane[:half] < BS // 2
    turned = pltpu.roll(cols, BS // 2, 1)
    low = jnp.where(side, cols[:half], turned[half:])
    high = jnp.where(side, turned[:half], cols[half:])
    me = ocn_ref[0]
    for k, send in zip(ks, sends):
        send[0 : 3 * ice, :] = out_ref[...]
        send[3 * ice :, :] = jnp.where((me ^ k) == me + 1, high, low)


def forward(lst, ocn, n_ocn, surf, weights, tracers, ice):
    planes, nbl = surf.shape[:2]
    _, levels, height, across = tracers.shape
    assert 4 * levels == BS and height == ice
    edge = jax.ShapeDtypeStruct((2 * levels * (across // BS), BS), F32)
    ks = edge_partners(n_ocn)
    send = jax.ShapeDtypeStruct((3 * ice + height // 2, BS), F32)
    return pl.pallas_call(
        functools.partial(forward_kernel, n_ocn),
        in_specs=[SM, SM, VM, ANY, VM],
        out_specs=[VM] * (3 + len(ks)),
        out_shape=[jax.ShapeDtypeStruct((3 * ice, BS), F32), edge, edge] + [send] * len(ks),
        scratch_shapes=[
            pltpu.VMEM((planes * nbl, BS), F32),
            pltpu.VMEM((ice, 4, BS), F32),
            pltpu.VMEM((FWD_SLOTS, BS, BS), BF16),
            pltpu.SemaphoreType.DMA((FWD_SLOTS,)),
        ],
        compiler_params=params(12),
        name="forward",
    )(lst, ocn, surf, in_hbm(weights), tracers)


def icerows_kernel(u_ref, wind_ref, rate_ref, strength_ref, x_ref):
    ice = rate_ref.shape[0]
    for r in range(ice):
        for c in range(2):
            x_ref[2 + c, r : r + 1, :] = u_ref[c : c + 1, r * BS : (r + 1) * BS]
            x_ref[c, r : r + 1, :] = wind_ref[c : c + 1, r * BS : (r + 1) * BS]
    rate = rate_ref[...]
    for c in range(2):
        x_ref[c] = rate * x_ref[2 + c] + x_ref[c]
    x_ref[4] = rate
    x_ref[5] = strength_ref[...]


def ice_rows(u, wind, rate, strength):
    return pl.pallas_call(
        icerows_kernel,
        in_specs=[VM] * 4,
        out_specs=VM,
        out_shape=jax.ShapeDtypeStruct((6,) + rate.shape, F32),
        compiler_params=params(2),
        name="icerows",
    )(u, wind, rate, strength)


def combine_kernel(ocn_ref, *refs):
    parts = refs[:-4]
    rows_ref, x_ref, rem_ref, cols_ref = refs[-4:]
    me, n = ocn_ref[0], len(parts)
    ice = rem_ref.shape[1]
    vals = [[p[c * ice : (c + 1) * ice, :] for c in range(3)] for p in parts]
    while len(vals) > 1:
        vals = [[x + y for x, y in zip(a, b)] for a, b in zip(vals[0::2], vals[1::2])]
    x_ref[...] = rows_ref[...]
    for c in range(3):
        rem_ref[c] = vals[0][c]
    for c in range(2):
        x_ref[c] = rows_ref[c] + vals[0][1 + c]
    to_east = jnp.where(me < n - 1, me ^ (me + 1), 0)
    to_west = jnp.where(me > 0, me ^ (me - 1), 0)
    east = jnp.zeros((cols_ref.shape[0] // 2, BS), F32)
    west = east
    for k in edge_partners(n):
        east = jnp.where(to_east == k, parts[k][3 * ice :, :], east)
        west = jnp.where(to_west == k, parts[k][3 * ice :, :], west)
    east = jnp.concatenate([east, pltpu.roll(east, BS // 2, 1)], axis=0)
    west = jnp.concatenate([pltpu.roll(west, BS // 2, 1), west], axis=0)
    lane = lax.broadcasted_iota(jnp.int32, cols_ref.shape, 1)
    cols_ref[...] = jnp.where(lane < BS // 2, east, west)


def combine(ocn, parts, rows):
    ice = rows.shape[1]
    return pl.pallas_call(
        combine_kernel,
        in_specs=[SM] + [VM] * (len(parts) + 1),
        out_specs=[VM, VM, VM],
        out_shape=[
            jax.ShapeDtypeStruct((6, ice, BS), F32),
            jax.ShapeDtypeStruct((3, ice, BS), F32),
            jax.ShapeDtypeStruct((ice, BS), F32),
        ],
        compiler_params=params(2),
        name="combine",
    )(ocn, *parts, rows)


def solve_kernel(halves, list_ref, me_ref, x_ref, rem_ref, row0_ref, rown_ref, w_hbm, *refs):
    groups_n, _, ice, _ = x_ref.shape
    outs = refs[:groups_n]
    ice_ref, fin, flux, back, buf, sems = refs[groups_n:]
    entries = w_hbm.shape[0]
    room = entries + UNROLL
    per_block = entries // ice
    nbl = outs[0].shape[0] // 3
    count = list_ref[2 * room]
    groups = lax.div(count + UNROLL - 1, UNROLL)

    def compute(base, slot):
        for q in range(UNROLL):
            e = list_ref[base + q]
            s = jnp.where(base + q < count, flux[lax.div(e, per_block)], 0.0).astype(BF16)
            part = lax.dot_general(
                s, buf[slot + q], (((1,), (0,)), ((), ())), preferred_element_type=F32
            )
            tile, place = place_of(list_ref[room + base + q], nbl // halves, halves)
            k = tile - me_ref[0]
            at = jnp.where(k < 0, k + groups_n, k) * nbl + place
            for f in range(3):
                back[f, pl.ds(at, 1), :] = back[f, pl.ds(at, 1), :] + part[f : f + 1]

    start, loop = stream_weights(list_ref, groups, w_hbm, buf, sems, compute)
    start()
    back[...] = jnp.zeros_like(back)

    n_rows = groups_n * ice
    total = 2.0 * n_rows * BS

    def plane(c):
        return jnp.concatenate([x_ref[a, c] for a in range(groups_n)], axis=0)

    base = [plane(0), plane(1)]
    current = [plane(2), plane(3)]
    rate1 = plane(4) + 1.0
    strength = plane(5)
    strength2 = 2.0 * strength
    lane = lax.broadcasted_iota(jnp.int32, (n_rows, BS), 1)
    corner = lax.broadcasted_iota(jnp.int32, (8, BS), 0) * BS + lane[:8]

    def picard(u):
        left, right = [], []
        for z in u:
            a = pltpu.roll(z, 1, 1)
            a = jnp.where(lane == 0, pltpu.roll(a, 1, 0), a)
            left.append(jnp.concatenate([jnp.where(corner == 0, 0.0, a[:8]), a[8:]], axis=0))
            a = pltpu.roll(z, BS - 1, 1)
            a = jnp.where(lane == BS - 1, pltpu.roll(a, n_rows - 1, 0), a)
            end = jnp.where(corner == 8 * BS - 1, 0.0, a[n_rows - 8 :])
            right.append(jnp.concatenate([a[: n_rows - 8], end], axis=0))
        dx = right[0] - left[0]
        dy = right[1] - left[1]
        d = dx * dx + dy * dy + 1.0
        q = d * lax.rsqrt(d)
        inverse = 1.0 / (rate1 * q + strength2)
        return [(base[c] * q + strength * (left[c] + right[c])) * inverse for c in range(2)]

    def dot(a, b):
        return jnp.sum(a[0] * b[0] + a[1] * b[1], keepdims=True) / total

    gvals, fvals, df, dg, gram, norms = [], [], [], [], {}, []
    for step in range(ITERS):
        gnew = picard(current)
        f = [gnew[c] - current[c] for c in range(2)]
        if step == 0:
            gvals, fvals = gnew, f
            current = gnew
            continue
        df.append([f[c] - fvals[c] for c in range(2)])
        dg.append([gnew[c] - gvals[c] for c in range(2)])
        gvals, fvals = gnew, f
        j = step - 1
        for i in range(j + 1):
            gram[i, j] = dot(df[i], df[j])
        norms.append(jnp.sqrt(gram[j, j] + 1e-06))
        used = list(range(max(0, step - DEPTH), step))
        m = len(used)
        a = [[None] * m for _ in range(m)]
        for p in range(m):
            for q in range(p + 1):
                i, k = used[q], used[p]
                a[p][q] = gram[i, k] / (norms[i] * norms[k])
            a[p][p] = a[p][p] + 0.1
        h = [dot(df[i], f) / norms[i] for i in used]
        d = [None] * m
        low = [[None] * m for _ in range(m)]
        y = [None] * m
        for p in range(m):
            acc = h[p]
            for q in range(p):
                v = a[p][q]
                for s in range(q):
                    v = v - low[p][s] * low[q][s] * d[s]
                low[p][q] = v / d[q]
                acc = acc - low[p][q] * y[q]
            v = a[p][p]
            for s in range(p):
                v = v - low[p][s] * low[p][s] * d[s]
            d[p] = v
            y[p] = acc
        coef = [None] * m
        for p in reversed(range(m)):
            v = y[p] / d[p]
            for q in range(p + 1, m):
                v = v - low[q][p] * coef[q]
            coef[p] = v
        current = list(gnew)
        for p, i in enumerate(used):
            scale = coef[p] / norms[i]
            for c in range(2):
                current[c] = current[c] - scale * dg[i][c]
    fin[0] = current[0]
    fin[1] = current[1]
    mine = pl.multiple_of(me_ref[0] * ice, ice)
    own = [fin[c, pl.ds(mine, ice), :] for c in range(2)]
    planes = [own[0] - rem_ref[1], own[1] - rem_ref[2], rem_ref[0]]
    for r in range(ice):
        for c in range(2):
            ice_ref[c : c + 1, r * BS : (r + 1) * BS] = own[c][r : r + 1]
        for f in range(3):
            flux[r, f : f + 1, :] = planes[f][r : r + 1]
        flux[r, 3:4, :] = jnp.zeros((1, BS), F32)
    loop()
    for k in range(groups_n):
        for f in range(3):
            outs[k][f * nbl : (f + 1) * nbl, :] = back[f, k * nbl : (k + 1) * nbl, :]
    outs[1][3 * nbl :, :] = rown_ref[...]
    outs[groups_n - 1][3 * nbl :, :] = row0_ref[...]


def solve(lst, me, x, rem, row0, rown, weights, nbl, halves):
    groups_n, _, ice, _ = x.shape
    assert groups_n > 2
    extra = [row0.shape[0] if k in (1, groups_n - 1) else 0 for k in range(groups_n)]
    chunks = [jax.ShapeDtypeStruct((3 * nbl + e, BS), F32) for e in extra]
    return pl.pallas_call(
        functools.partial(solve_kernel, halves),
        in_specs=[SM, SM, VM, VM, VM, VM, ANY],
        out_specs=[VM] * (groups_n + 1),
        out_shape=chunks + [jax.ShapeDtypeStruct((2, ice * BS), F32)],
        scratch_shapes=[
            pltpu.VMEM((2, groups_n * ice, BS), F32),
            pltpu.VMEM((ice, 4, BS), F32),
            pltpu.VMEM((3, groups_n * nbl, BS), F32),
            pltpu.VMEM((BWD_SLOTS, BS, BS), BF16),
            pltpu.SemaphoreType.DMA((BWD_SLOTS,)),
        ],
        compiler_params=params(14),
        name="solve",
    )(lst, me, x, rem, row0, rown, in_hbm(weights))


def finish_kernel(*refs):
    chunks = refs[:-6]
    level_ref, _, flux_ref, out_hbm, buf, sem = refs[-6:]
    height, across = level_ref.shape
    put = pltpu.make_async_copy(buf, out_hbm.at[0, 0], sem)
    for f in (2, 0, 1):
        for h in range(across // BS):
            at = (f * (across // BS) + h) * height
            v = chunks[0][at : at + height, :]
            for c in chunks[1:]:
                v = v + c[at : at + height, :]
            flux_ref[f, :, h * BS : (h + 1) * BS] = v
            if f == 2:
                cols = slice(h * BS, (h + 1) * BS)
                buf[:, cols] = level_ref[:, cols] + 0.5 * v
        if f == 2:
            put.start()
    put.wait()


def finish(chunks, level, tracers_next):
    height, across = level.shape
    return pl.pallas_call(
        finish_kernel,
        in_specs=[VM] * (len(chunks) + 1) + [ANY],
        out_specs=[VM, ANY],
        out_shape=[
            jax.ShapeDtypeStruct((3, height, across), F32),
            jax.ShapeDtypeStruct(tracers_next.shape, F32),
        ],
        scratch_shapes=[pltpu.VMEM((height, across), F32), pltpu.SemaphoreType.DMA(())],
        input_output_aliases={len(chunks) + 1: 1},
        compiler_params=params(4),
        name="finish",
    )(*chunks, level, in_hbm(tracers_next))


def coupled_step(
    tracers,
    velocity,
    remap_weights,
    remap_blocks,
    remap_count,
    ice_velocity,
    ice_mass_rate,
    ice_strength,
    wind_stress,
):
    n_grp = lax.axis_size("grp")
    n_ocn = lax.axis_size("ocn")
    column = lax.axis_index("ocn")
    me = lax.axis_index("grp")
    height, across = tracers.shape[2:]
    halves = across // BS
    nbl = height * halves
    ice, per_block = remap_blocks.shape
    weights = remap_weights.reshape(ice * per_block, BS, BS)

    ocn = column.reshape(1)
    surf, lst = pack_surface(n_grp, remap_blocks.T, remap_count, ocn, tracers, velocity)
    surf = lax.all_gather(surf, "grp", axis=0, tiled=True)
    assert n_ocn & (n_ocn - 1) == 0
    part, row0, rown, *sends = forward(lst, ocn, n_ocn, surf, weights, tracers, ice)
    sends = dict(zip(edge_partners(n_ocn), sends))
    parts = [part]
    for k in range(1, n_ocn):
        pairs = [(i, i ^ k) for i in range(n_ocn)]
        parts.append(lax.ppermute(sends.get(k, part), "ocn", pairs))
    rows = ice_rows(
        ice_velocity,
        wind_stress,
        ice_mass_rate.reshape(ice, BS),
        ice_strength.reshape(ice, BS),
    )
    x, rem, cols = combine(ocn, parts, rows)
    xg = lax.all_gather(x, "grp", axis=0)
    *chunks, ice_final = solve(
        lst, me.reshape(1), xg, rem, row0, rown, weights, nbl, halves
    )
    moved = {0: chunks[0]}
    for k in [1, n_grp - 1] + list(range(2, n_grp - 1)):
        ring = [(i, (i + k) % n_grp) for i in range(n_grp)]
        moved[k] = lax.ppermute(chunks[k], "grp", ring)
    tracers_next, level = stencil(me.reshape(1), n_grp, tracers, velocity, moved[1], moved[n_grp - 1], cols)
    surface_flux, tracers_next = finish([moved[k] for k in range(n_grp)], level, tracers_next)
    return tracers_next, surface_flux, ice_final


def solution(mesh):
    return jax.shard_map(
        coupled_step,
        mesh=mesh,
        in_specs=(
            P(None, None, "grp", "ocn"),
            P(None, None, "grp", "ocn"),
            P("grp", None, None, None),
            P("grp", None),
            P("grp"),
            P(None, "grp"),
            P("grp"),
            P("grp"),
            P(None, "grp"),
        ),
        out_specs=(P(None, None, "grp", "ocn"), P(None, "grp", "ocn"), P(None, "grp")),
        check_vma=False,
    )
```
